32 devices in a mesh: replica: 2 (over x), fsdp: 16 (over z, y, core).
Axes of the slice: x: 2, y: 2, z: 4, core: 2. Of those that a mesh axis runs over, the one named last changes fastest.
Arguments:
- tokens: bfloat16 [16384, 768], P(('replica', 'fsdp')), may hold values from -6 to 6
- cotangent: bfloat16 [16384, 768], P(('replica', 'fsdp')), may hold values from -6 to 6
- qkv_weight: bfloat16 [768, 2304], P('fsdp'), may hold values from -0.21875 to 0.21875
- qkv_bias: bfloat16 [2304], P('fsdp'), may hold values from -3 to 3
- proj_weight: bfloat16 [768, 768], P('fsdp'), may hold values from -1.75 to 1.75
- proj_bias: bfloat16 [768], P('fsdp'), may hold values from -3 to 3
- attn_gain: bfloat16 [768], P('fsdp'), may hold values from 0.5 to 1.5
- attn_shift: bfloat16 [768], P('fsdp'), may hold values from -3 to 3
- inner_weight: bfloat16 [768, 3072], P('fsdp'), may hold values from -0.21875 to 0.21875
- inner_bias: bfloat16 [3072], P('fsdp'), may hold values from -3 to 3
- outer_weight: bfloat16 [3072, 768], P('fsdp'), may hold values from -0.21875 to 0.21875
- outer_bias: bfloat16 [768], P('fsdp'), may hold values from -3 to 3
- ffn_gain: bfloat16 [768], P('fsdp'), may hold values from 0.5 to 1.5
- ffn_shift: bfloat16 [768], P('fsdp'), may hold values from -3 to 3
- random_dirs: bfloat16 [12, 64, 256], replicated, may hold values from -5 to 5
- seq_lengths: int32 [2, 16, 4], P('replica', 'fsdp'), may hold values from 1 to 256, 448 in all within a row
- deal_order: int32 [2, 16], P('replica'), may hold values from 0 to 15, each once within a row
Outputs:
- layer_out: bfloat16 [16384, 768], P(('replica', 'fsdp'))
- tokens_grad: bfloat16 [16384, 768], P(('replica', 'fsdp'))
- qkv_weight_grad: float32 [768, 2304], P('fsdp')
- qkv_bias_grad: float32 [2304], P('fsdp')
- proj_weight_grad: float32 [768, 768], P('fsdp')
- proj_bias_grad: float32 [768], P('fsdp')
- attn_gain_grad: float32 [768], P('fsdp')
- attn_shift_grad: float32 [768], P('fsdp')
- inner_weight_grad: float32 [768, 3072], P('fsdp')
- inner_bias_grad: float32 [3072], P('fsdp')
- outer_weight_grad: float32 [3072, 768], P('fsdp')
- outer_bias_grad: float32 [768], P('fsdp')
- ffn_gain_grad: float32 [768], P('fsdp')
- ffn_shift_grad: float32 [768], P('fsdp')
The draws below stay inside these ranges and needn't reach their ends.
Inputs may be any that keep to these rules, and one draw needn't show every extreme that they name: `seq_lengths`: the 4 sequences of each dealt buffer lie one after another in its first 448 rows, the longest of each exactly 256 rows; the last 64 rows are padding. `deal_order`: each row is a permutation of the 16 buffers of one replica group.
All inputs are finite; a program needn't handle non-finite values.
Results may differ from the reference program's by a relative error of at most 0.03.
Values may be sent and summed in bfloat16 or wider, within the bound.
A program may use at most 128 MiB of HBM per device.

```python
import math
import jax
import jax.numpy as jnp
import numpy as np
from jax import lax

D = 768
H = 12
DH = 64
FF = 3072
M = 256
TOK_DEV = 512
SEQ_DEV = 4
FILLED = 448
LMAX = 256
PIECE = 32
TOKENS = 16384
N_REPLICA = 2
N_FSDP = 16


def block_scale(rng, extent, pieces, least, high):
    loudness = 1.0
    for dim, shards_of in pieces:
        draws = jax.random.uniform(jax.random.fold_in(jax.random.fold_in(rng, 6), dim), (shards_of,), jnp.float32, least / len(pieces), high / len(pieces))
        loudness = loudness * jnp.repeat(jnp.exp(draws), extent[dim] // shards_of).reshape((-1,) + (1,) * (len(extent) - 1 - dim))
    return loudness


def split_up(number_of, total, reach, slope):
    portions = [(1 << 20) // math.isqrt(grade ** slope) + 1 for grade in range(2, number_of + 1)]
    surplus, counts = total - reach - (number_of - 1), [1] * (number_of - 1)
    while surplus > 0:
        candidates = [i for i in range(number_of - 1) if counts[i] < reach]
        pool, left = sum([portions[i] for i in candidates]), surplus
        for i in candidates:
            addition = min(reach - counts[i], max(1, left * portions[i] // pool), surplus)
            counts[i] = counts[i] + addition
            surplus = surplus - addition
    return np.array([reach] + counts)


def ragged(stream_key, amount, total, most, slope):
    if amount == 2:
        one = jax.random.randint(stream_key, (), max(1, total - most), min(most, total - 1) + 1)
        return jnp.stack([one, total - one])
    sizes = jnp.asarray(split_up(amount, total, most, slope), jnp.int32)
    pairs = (amount - 1) // 2
    source_of, receiver = sizes[1:1 + 2 * pairs:2], sizes[2:2 + 2 * pairs:2]
    margin = jnp.minimum(source_of - 1, most - receiver)
    shifted = jax.random.randint(jax.random.fold_in(stream_key, 1), (pairs,), 0, 1 << 20) % (margin + 1)
    sizes = sizes.at[1:1 + 2 * pairs:2].set(source_of - shifted).at[2:2 + 2 * pairs:2].set(receiver + shifted)
    return sizes[jax.random.permutation(jax.random.fold_in(stream_key, 2), amount)]


def noise(own_key, extent, deviation, most, shards=(), kind=jnp.bfloat16):
    factor_of = block_scale(own_key, extent, shards, -0.22, 0.18) if shards else 1.0
    array = jax.random.normal(own_key, extent, jnp.float32) * deviation * factor_of
    return jnp.minimum(jnp.maximum(array, -most), most).astype(kind)


def setup_inputs(seed: int = 0) -> dict:
    streams_of = jax.random.split(jax.random.key(seed), 18)
    return {
        "tokens": noise(streams_of[0], (TOKENS, D), 1.0, 6.0, ((0, 32),)),
        "cotangent": noise(streams_of[1], (TOKENS, D), 1.0, 6.0, ((0, 32),)),
        "qkv_weight": noise(streams_of[2], (D, 3 * D), D ** -0.5, 0.21875, ((0, 16),)),
        "qkv_bias": noise(streams_of[3], (3 * D,), 0.5, 3.0, ((0, 16),)),
        "proj_weight": noise(streams_of[4], (D, D), (max(D // 64, 8)) ** -0.5, 1.75, ((0, 16),)),
        "proj_bias": noise(streams_of[5], (D,), 0.3, 3.0, ((0, 16),)),
        "attn_gain": jnp.clip(1.0 + 0.1 * jax.random.normal(streams_of[6], (D,), jnp.float32), 0.5, 1.5).astype(jnp.bfloat16),
        "attn_shift": noise(streams_of[7], (D,), 0.3, 3.0, ((0, 16),)),
        "inner_weight": noise(streams_of[8], (D, FF), D ** -0.5, 0.21875, ((0, 16),)),
        "inner_bias": noise(streams_of[9], (FF,), 0.5, 3.0, ((0, 16),)),
        "outer_weight": noise(streams_of[10], (FF, D), (FF // 4) ** -0.5, 0.21875, ((0, 16),)),
        "outer_bias": noise(streams_of[11], (D,), 0.3, 3.0, ((0, 16),)),
        "ffn_gain": jnp.clip(1.0 + 0.1 * jax.random.normal(streams_of[12], (D,), jnp.float32), 0.5, 1.5).astype(jnp.bfloat16),
        "ffn_shift": noise(streams_of[13], (D,), 0.3, 3.0, ((0, 16),)),
        "random_dirs": noise(streams_of[14], (H, DH, M), 1.0, 5.0),
        "seq_lengths": jax.vmap(lambda own: ragged(own, SEQ_DEV, FILLED, LMAX, 1))(jax.random.split(streams_of[15], N_REPLICA * N_FSDP)).reshape((N_REPLICA, N_FSDP, SEQ_DEV)).astype(jnp.int32),
        "deal_order": jax.vmap(lambda own: jax.random.permutation(own, N_FSDP))(jax.random.split(streams_of[16], N_REPLICA)).reshape((N_REPLICA, N_FSDP)).astype(jnp.int32),
    }


@jax.custom_vjp
def low(v):
    return lax.optimization_barrier(v.astype(jnp.bfloat16)).astype(jnp.float32)

@jax.custom_vjp
def low_back(v):
    return v

def low_keep(v):
    return (low(v), None)

def low_pass(kept, grad):
    return (grad,)

def back_keep(v):
    return (v, None)

def back_low(kept, grad):
    return (low(grad),)
low.defvjp(low_keep, low_pass)
low_back.defvjp(back_keep, back_low)
EPSILON = 1e-06
HIGHEST = lax.Precision.HIGHEST

def matrix_product(left, right):
    return jnp.dot(left, right, precision=HIGHEST, preferred_element_type=jnp.float32)

def layer_norm(summed, gain_vec, shift_vec):
    centered = summed - lax.optimization_barrier(jnp.mean(summed, -1, keepdims=True))
    inv_std = lax.rsqrt(lax.optimization_barrier(jnp.mean(centered * centered, -1, keepdims=True)) + EPSILON)
    return centered * inv_std * gain_vec + shift_vec

def feature_map(scaled, directions):
    project = low_back(jnp.einsum('rhd,hdm->rhm', scaled, directions, precision=HIGHEST))
    return low(jnp.exp(project - 0.5 * lax.optimization_barrier(jnp.sum(scaled * scaled, -1, keepdims=True))))

def forward(params, inputs, select, valid_rows, directions):
    weight_qkv, bias_qkv, weight_proj, bias_proj, gain_attn, shift_attn, weight_inner, bias_inner, weight_outer, bias_outer, gain_ffn, shift_ffn = params
    row_count = inputs.shape[0]
    qkv_act = low_back(matrix_product(inputs, weight_qkv) + bias_qkv)
    feature_scale = DH ** (-0.25)
    query_part = low(qkv_act[:, :D] * feature_scale).reshape(row_count, H, DH)
    key_part = low(qkv_act[:, D:2 * D] * feature_scale).reshape(row_count, H, DH)
    value_part = low(qkv_act[:, 2 * D:]).reshape(row_count, H, DH)
    query_feat = feature_map(query_part, directions)
    key_feat = feature_map(key_part, directions)
    masked_keys = select[:, :, None, None] * key_feat[:, None]
    masked_query = select[:, :, None, None] * query_feat[:, None]
    kv_state = low(low_back(jnp.einsum('rshm,rhe->shme', masked_keys, value_part, precision=HIGHEST)))
    key_total = low(low_back(lax.optimization_barrier(jnp.sum(masked_keys, axis=0))))
    numerator = low_back(jnp.einsum('rshm,shme->rhe', masked_query, kv_state, precision=HIGHEST))
    denominator = low_back(jnp.einsum('rshm,shm->rh', masked_query, key_total, precision=HIGHEST))
    context = low((numerator / denominator[:, :, None]).reshape(row_count, D))
    attn_out = low_back(matrix_product(context, weight_proj) + bias_proj)
    hidden = layer_norm(inputs + attn_out, gain_attn, shift_attn)
    inner_act = low_back(matrix_product(low(hidden), weight_inner) + bias_inner)
    gelu_low = low(jax.nn.gelu(inner_act, approximate=False))
    outer_act = low_back(matrix_product(gelu_low, weight_outer) + bias_outer)
    return layer_norm(hidden + outer_act, gain_ffn, shift_ffn) * valid_rows

def reference(tokens, cotangent, qkv_weight, qkv_bias, proj_weight, proj_bias, attn_gain, attn_shift, inner_weight, inner_bias, outer_weight, outer_bias, ffn_gain, ffn_shift, random_dirs, seq_lengths, deal_order):
    params = tuple((tensor.astype(jnp.float32) for tensor in (qkv_weight, qkv_bias, proj_weight, proj_bias, attn_gain, attn_shift, inner_weight, inner_bias, outer_weight, outer_bias, ffn_gain, ffn_shift)))
    directions = random_dirs.astype(jnp.float32)
    replica_ids = jnp.arange(N_REPLICA, dtype=jnp.int32)[:, None]
    deal_index = deal_order.astype(jnp.int32)

    def to_dealt(given):
        shaped = given.astype(jnp.float32).reshape(N_REPLICA, N_FSDP, N_FSDP, PIECE, D).transpose(0, 2, 1, 3, 4)
        return shaped[replica_ids, deal_index].reshape(N_REPLICA * N_FSDP, TOK_DEV, D)
    dealt_x = to_dealt(tokens)
    dealt_g = to_dealt(cotangent)
    dealt_len = seq_lengths.astype(jnp.int32).reshape(N_REPLICA * N_FSDP, SEQ_DEV)
    position = jnp.arange(TOK_DEV, dtype=jnp.int32)
    slot_ids = jnp.arange(SEQ_DEV + 1, dtype=jnp.int32)

    def buffer_step(carried, inputs_now):
        buffer_x, buffer_grad, lengths_now = inputs_now
        seq_ends = jnp.cumsum(lengths_now).astype(jnp.int32)
        segment = lax.optimization_barrier(jnp.sum((position[:, None] >= seq_ends[None, :]).astype(jnp.int32), axis=1)).astype(jnp.int32)
        select = (segment[:, None] == slot_ids[None, :]).astype(jnp.float32)
        valid_rows = (segment < SEQ_DEV).astype(jnp.float32)[:, None]
        result, pullback = jax.vjp(lambda weights, source: forward(weights, source, select, valid_rows, directions), params, buffer_x)
        weight_grads, input_grad = pullback(buffer_grad)
        carried = jax.tree.map(lambda summed, addend: summed + addend, carried, weight_grads)
        return (carried, (result, input_grad))
    start = tuple((jnp.zeros(tensor.shape, jnp.float32) for tensor in params))
    totals, (dealt_out, dealt_grad) = lax.scan(buffer_step, start, (dealt_x, dealt_g, dealt_len))

    def to_given(dealt):
        placed = jnp.zeros((N_REPLICA, N_FSDP, N_FSDP, PIECE, D), jnp.float32)
        placed = placed.at[replica_ids, deal_index].set(dealt.reshape(N_REPLICA, N_FSDP, N_FSDP, PIECE, D))
        return placed.transpose(0, 2, 1, 3, 4).reshape(TOKENS, D)
    layer_out = to_given(dealt_out).astype(jnp.bfloat16)
    tokens_grad = to_given(dealt_grad).astype(jnp.bfloat16)
    return (layer_out, tokens_grad, totals[0], totals[1], totals[2], totals[3], totals[4], totals[5], totals[6], totals[7], totals[8], totals[9], totals[10], totals[11])
```

```python
from functools import partial

import jax
import jax.numpy as jnp
from jax import lax
from jax.experimental import pallas as pl
from jax.experimental.pallas import tpu as pltpu
from jax.sharding import PartitionSpec as P

EPSILON = 1e-06
ANY = pl.BlockSpec(memory_space=pl.ANY)
VMEM = pl.BlockSpec(memory_space=pltpu.VMEM)
MESH = pl.DeviceIdType.MESH
DMA = pltpu.SemaphoreType.DMA


class Place:
    def __init__(self, n, replicas):
        self.n, self.replicas = n, replicas
        self.nz = 4 if n % 8 == 0 else n // 2
        self.ny = n // (2 * self.nz)
        self.chips = n // 2
        self.f = lax.axis_index("fsdp")
        self.r = lax.axis_index("replica")
        self.core = self.f % 2
        chip = self.f // 2
        y, z = chip % self.ny, chip // self.ny
        odd = y % 2
        self.pos = y * self.nz + z * (1 - odd) + (self.nz - 1 - z) * odd
        self.role = self.r % 2

    def dev(self, pos, core):
        pos = (pos + 2 * self.chips) % self.chips
        y, t = pos // self.nz, pos % self.nz
        odd = y % 2
        z = t * (1 - odd) + (self.nz - 1 - t) * odd
        return (z * self.ny + y) * 2 + core

    def peer(self, f):
        return (self.r, f)

    def ring(self, direction):
        return self.peer(self.dev(self.pos + (1 if direction == 0 else -1), self.core))

    def mate(self):
        return self.peer(self.f + 1 - 2 * self.core)

    def across(self):
        return (self.r + 1 - 2 * self.role, self.f)

    def greet(self):
        barrier = pltpu.get_barrier_semaphore()

        @pl.loop(1, self.n)
        def _(k):
            pl.semaphore_signal(barrier, inc=1, device_id=self.peer((self.f + k) % self.n), device_id_type=MESH)

        @pl.loop(1, self.replicas)
        def _(k):
            pl.semaphore_signal(barrier, inc=1, device_id=((self.r + k) % self.replicas, self.f), device_id_type=MESH)

        pl.semaphore_wait(barrier, self.n - 1 + self.replicas - 1)


def remote(src, dst, send, recv, device):
    return pltpu.make_async_remote_copy(
        src_ref=src, dst_ref=dst, send_sem=send, recv_sem=recv, device_id=device, device_id_type=MESH
    )


class Exchange:
    def __init__(self, place, send, recv, sems):
        self.place, self.send, self.recv = place, send, recv
        self.out_sem, self.in_sem, self.own_sem = sems

    def copy(self, target):
        me = self.place.f
        return remote(
            self.send.at[target], self.recv.at[me], self.out_sem, self.in_sem, self.place.peer(target)
        )

    def own(self):
        me = self.place.f
        return pltpu.make_async_copy(self.send.at[me], self.recv.at[me], self.own_sem)

    def start(self):
        self.own().start()

        @pl.loop(1, self.place.n)
        def _(k):
            self.copy((self.place.f + k) % self.place.n).start()

    def finish(self):
        rest = self.recv.at[pl.ds(0, self.place.n - 1)]
        pltpu.make_async_copy(rest, rest, self.out_sem).wait()
        pltpu.make_async_copy(rest, rest, self.in_sem).wait()
        self.own().wait()


class Gather:
    def __init__(self, place, shard, full, sems):
        self.place, self.shard, self.full = place, shard, full
        self.ring_in, self.across_in, self.flat = sems
        self.rows, self.cols = shard.shape
        split = self.rows % 48 == 0 and place.replicas % 2 == 0
        self.third = self.rows // 3 if split else 0
        self.main = self.rows - self.third
        self.half = self.cols // 2

    def box(self, ref, owner, offset, count, direction):
        row = offset if owner is None else owner * self.rows + offset
        if owner is not None or not isinstance(row, int):
            row = pl.multiple_of(row, 8)
        return ref.at[pl.ds(row, count), pl.ds(direction * self.half, self.half)]

    def origin(self, s, direction):
        return self.place.pos - s if direction == 0 else self.place.pos + s

    def ring_copy(self, s, direction, own=False):
        owner = self.place.dev(self.origin(s, direction), self.place.core)
        lead = self.place.role * self.third
        dst = self.box(self.full, owner, lead, self.main, direction)
        src = self.box(self.shard, None, lead, self.main, direction) if own else dst
        return remote(src, dst, self.flat.at[0], self.ring_in.at[s, direction], self.place.ring(direction))

    def mate_copy(self, s, direction, lead, count):
        owner = self.place.dev(self.origin(s, direction), self.place.core)
        part = self.box(self.full, owner, lead, count, direction)
        return remote(part, part, self.flat.at[1], self.flat.at[2], self.place.mate())

    def across_copy(self, s, direction, arriving=False):
        owner = self.place.dev(self.origin(s, direction), self.place.core)
        role = 1 - self.place.role if arriving else self.place.role
        part = self.box(self.full, owner, role * 2 * self.third, self.third, direction)
        return remote(part, part, self.flat.at[3], self.across_in.at[s - 1, direction], self.place.across())

    def own_copy(self):
        row = pl.multiple_of(self.place.f * self.rows, 8)
        return pltpu.make_async_copy(self.shard, self.full.at[pl.ds(row, self.rows)], self.flat.at[4])

    def start(self):
        for direction in range(2):
            self.ring_copy(0, direction, own=True).start()
        row = pl.multiple_of(self.place.f * self.rows, 8)
        remote(
            self.shard, self.full.at[pl.ds(row, self.rows)], self.flat.at[1], self.flat.at[2], self.place.mate()
        ).start()
        self.own_copy().start()

    def step(self, s, last=False):
        for direction in range(2):
            owner = self.place.dev(self.origin(s, direction), self.place.core)
            lead = self.place.role * self.third
            part = self.box(self.full, owner, lead, self.main, direction)
            remote(part, part, self.flat.at[0], self.ring_in.at[s - 1, direction], self.place.ring(direction)).wait_recv()
            if not last:
                self.ring_copy(s, direction).start()
            if self.third:
                self.across_copy(s, direction).start()
            self.mate_copy(s, direction, lead, self.main).start()

    def across_step(self, s):
        if self.third:
            for direction in range(2):
                self.across_copy(s, direction, arriving=True).wait_recv()
                self.mate_copy(s, direction, (1 - self.place.role) * 2 * self.third, self.third).start()

    def wait_rows(self, count, index):
        part = self.full.at[pl.ds(0, count)]
        pltpu.make_async_copy(part, part, self.flat.at[index]).wait()

    def finish(self):
        hops = self.place.chips - 1
        self.wait_rows(hops * self.main, 0)
        self.wait_rows(self.place.chips * self.rows, 1)
        self.wait_rows(self.place.chips * self.rows, 2)
        if self.third:
            self.wait_rows(hops * self.third, 3)
        self.own_copy().wait()


def gather_kernel(n, replicas, weights, exchanges, *refs):
    refs = list(refs)
    take = lambda count: [refs.pop(0) for _ in range(count)]
    shards, sends = take(weights), take(exchanges)
    fulls, recvs = take(weights), take(exchanges)
    gather_sems = [take(3) for _ in range(weights)]
    exchange_sems = [take(3) for _ in range(exchanges)]
    place = Place(n, replicas)
    gathers = [Gather(place, *item) for item in zip(shards, fulls, gather_sems)]
    swaps = [Exchange(place, *item) for item in zip(sends, recvs, exchange_sems)]
    place.greet()
    for item in gathers:
        item.start()
    for item in swaps:
        item.start()
    hops = place.chips - 1

    for item in gathers:
        item.step(1, last=hops == 1)

    @pl.loop(2, hops)
    def _(s):
        for item in gathers:
            item.step(s)
        for item in gathers:
            item.across_step(s - 1)

    for item in gathers:
        item.step(hops, last=True)
    for item in gathers:
        item.across_step(hops - 1)
    for item in gathers:
        item.across_step(hops)
    for item in gathers:
        item.finish()
    for item in swaps:
        item.finish()


def gather_all(n, replicas, collective_id, shards, sends):
    hops = n // 2 - 1
    outs = [jax.ShapeDtypeStruct((n * a.shape[0], a.shape[1]), a.dtype) for a in shards]
    outs += [jax.ShapeDtypeStruct(a.shape, a.dtype) for a in sends]
    scratch = [DMA((hops, 2)), DMA((hops, 2)), DMA((5,))] * len(shards) + [DMA(()), DMA(()), DMA(())] * len(sends)
    return pl.pallas_call(
        partial(gather_kernel, n, replicas, len(shards), len(sends)),
        out_shape=outs,
        in_specs=[VMEM] * len(shards) + [ANY] * len(sends),
        out_specs=[ANY] * len(outs),
        scratch_shapes=scratch,
        compiler_params=pltpu.CompilerParams(collective_id=collective_id, has_side_effects=True),
        name="gather_all",
    )(*shards, *sends)


class Scatter:
    def __init__(self, place, grad, total, bufs, sems):
        self.place, self.grad, self.total = place, grad, total
        self.own, self.other, self.ringed, self.repl = bufs
        self.own_in, self.core_in, self.ring_in, self.repl_in, self.flat = sems
        self.rows, self.cols = total.shape
        self.half = self.cols // 2

    def rows_of(self, pos, core):
        row = pl.multiple_of(self.place.dev(pos, core) * self.rows, 8)
        return self.grad.at[pl.ds(row, self.rows)]

    def slot(self, pos):
        return (pos + 2 * self.place.chips) % self.place.chips

    def load(self, pos):
        k = self.slot(pos)
        return pltpu.make_async_copy(self.rows_of(pos, self.place.core), self.own.at[k], self.own_in.at[k])

    def give(self, pos):
        k = self.slot(pos)
        return remote(
            self.rows_of(pos, 1 - self.place.core), self.other.at[k], self.flat.at[0], self.core_in.at[k], self.place.mate()
        )

    def start(self):
        def one(k, _):
            pos = self.place.pos + ((k + 2) // 2) * (2 * (k % 2) - 1)
            self.load(pos).start()
            self.give(pos).start()
            return 0

        lax.fori_loop(0, self.place.chips - 1, one, 0)
        self.load(self.place.pos).start()
        self.give(self.place.pos).start()

    def merge(self, pos):
        k = self.slot(pos)
        self.load(pos).wait()
        self.give(pos).wait_recv()
        self.own[k] = (self.own[k].astype(jnp.float32) + self.other[k].astype(jnp.float32)).astype(jnp.bfloat16)

    def target(self, s, direction):
        return self.place.pos - 1 - s if direction == 0 else self.place.pos + 1 + s

    def cols_of(self, direction):
        return pl.ds(direction * self.half, self.half)

    def ring_copy(self, s, direction, first=False):
        cols = self.cols_of(direction)
        if first:
            src = self.own.at[self.slot(self.target(0, direction)), :, cols]
        else:
            src = self.ringed.at[s - 1, :, cols]
        return remote(src, self.ringed.at[s, :, cols], self.flat.at[1], self.ring_in.at[s, direction], self.place.ring(direction))

    def absorb(self, s, direction):
        cols = self.cols_of(direction)
        self.ring_copy(s, direction, first=True).wait_recv()
        k = self.slot(self.target(s + 1, direction))
        self.ringed[s, :, cols] = (
            self.ringed[s, :, cols].astype(jnp.float32) + self.own[k, :, cols].astype(jnp.float32)
        ).astype(jnp.bfloat16)

    def publish(self):
        hops = self.place.chips - 1
        last = self.ringed.at[hops - 1]

        def one(k, _):
            r = (self.place.r + k) % self.place.replicas
            remote(last, self.repl.at[self.place.r], self.flat.at[2], self.repl_in.at[0], (r, self.place.f)).start()
            return 0

        lax.fori_loop(1, self.place.replicas, one, 0)
        self.repl[self.place.r] = self.ringed[hops - 1]

    def finish(self):
        others = self.repl.at[pl.ds(0, self.place.replicas - 1)]
        pltpu.make_async_copy(others, others, self.repl_in.at[0]).wait()
        total = self.repl[0].astype(jnp.float32)
        for r in range(1, self.place.replicas):
            total = total + self.repl[r].astype(jnp.float32)
        self.total[...] = total
        pltpu.make_async_copy(others, others, self.flat.at[2]).wait()
        pltpu.make_async_copy(self.ringed, self.ringed, self.flat.at[1]).wait()
        pltpu.make_async_copy(self.other, self.other, self.flat.at[0]).wait()


def scatter_kernel(n, replicas, weights, exchanges, *refs):
    refs = list(refs)
    take = lambda count: [refs.pop(0) for _ in range(count)]
    grads, (small,), sends = take(weights), take(1), take(exchanges)
    totals, (small_total,), recvs = take(weights), take(1), take(exchanges)
    bufs = [take(4) for _ in range(weights)]
    small_in, small_group = take(2)
    sems = [take(5) for _ in range(weights)]
    small_sems = take(3)
    small_repl, = take(1)
    exchange_sems = [take(3) for _ in range(exchanges)]
    place = Place(n, replicas)
    scatters = [Scatter(place, *item) for item in zip(grads, totals, bufs, sems)]
    swaps = [Exchange(place, *item) for item in zip(sends, recvs, exchange_sems)]
    smalls = Exchange(place, small, small_in, small_sems)
    place.greet()
    hops = place.chips - 1
    for item in scatters:
        item.start()
    smalls.start()
    for item in scatters:
        item.merge(place.pos - 1)
        item.ring_copy(0, 0, first=True).start()
        item.merge(place.pos + 1)
        item.ring_copy(0, 1, first=True).start()
    for item in swaps:
        item.start()
    half = (place.chips - 2) // 2

    def early(s, _):
        for item in scatters:
            item.merge(place.pos - 2 - s)

            @pl.when(s < hops // 2 - 1)
            def _():
                item.merge(place.pos + 2 + s)

            for direction in range(2):
                item.absorb(s, direction)
                item.ring_copy(s + 1, direction).start()
        return 0

    def late(s, _):
        for item in scatters:
            for direction in range(2):
                item.absorb(s, direction)
                item.ring_copy(s + 1, direction).start()
        return 0

    lax.fori_loop(0, half, early, 0)
    lax.fori_loop(half, hops - 1, late, 0)
    smalls.finish()
    group = small_in[0]
    for k in range(1, n):
        group = group + small_in[k]
    small_group[place.r] = group

    def tell(k, _):
        r = (place.r + k) % replicas
        remote(small_group.at[place.r], small_group.at[place.r], small_repl.at[0], small_repl.at[1], (r, place.f)).start()
        return 0

    lax.fori_loop(1, replicas, tell, 0)
    for item in scatters:
        item.merge(place.pos)
        for direction in range(2):
            item.absorb(hops - 1, direction)
        item.publish()
    others = small_group.at[pl.ds(0, replicas - 1)]
    pltpu.make_async_copy(others, others, small_repl.at[1]).wait()
    total = small_group[0]
    for r in range(1, replicas):
        total = total + small_group[r]
    small_total[...] = total
    pltpu.make_async_copy(others, others, small_repl.at[0]).wait()
    for item in scatters:
        item.finish()
    for item in swaps:
        item.finish()


def scatter_all(n, replicas, collective_id, grads, small, sends):
    chips, hops = n // 2, n // 2 - 1
    outs = [jax.ShapeDtypeStruct((a.shape[0] // n, a.shape[1]), jnp.float32) for a in grads]
    outs += [jax.ShapeDtypeStruct(small.shape[1:], jnp.float32)]
    outs += [jax.ShapeDtypeStruct(a.shape, a.dtype) for a in sends]
    scratch = []
    for a in grads:
        block = (a.shape[0] // n, a.shape[1])
        scratch += [pltpu.VMEM((count,) + block, jnp.bfloat16) for count in (chips, chips, hops, replicas)]
    scratch += [pltpu.VMEM(small.shape, jnp.float32), pltpu.VMEM((replicas,) + small.shape[1:], jnp.float32)]
    scratch += [DMA((chips,)), DMA((chips,)), DMA((hops, 2)), DMA((1,)), DMA((3,))] * len(grads)
    scratch += [DMA(()), DMA(()), DMA(()), DMA((2,))] + [DMA(()), DMA(()), DMA(())] * len(sends)
    return pl.pallas_call(
        partial(scatter_kernel, n, replicas, len(grads), len(sends)),
        out_shape=outs,
        in_specs=[ANY] * (len(grads) + 1 + len(sends)),
        out_specs=[VMEM] * (len(grads) + 1) + [ANY] * len(sends),
        scratch_shapes=scratch,
        compiler_params=pltpu.CompilerParams(
            collective_id=collective_id, has_side_effects=True, vmem_limit_bytes=56 << 20
        ),
        name="scatter_all",
    )(*grads, small, *sends)


def pack_small(vectors, rows):
    joined = jnp.concatenate(vectors, axis=-1)
    room = rows * 128 - joined.shape[-1]
    joined = jnp.pad(joined, [(0, 0)] * (joined.ndim - 1) + [(0, room)])
    return joined.reshape(joined.shape[:-1] + (rows, 128))


def unpack_small(packed, sizes):
    flat = packed.reshape(packed.shape[:-2] + (-1,))
    parts, at = [], 0
    for size in sizes:
        parts.append(flat[..., at : at + size])
        at += size
    return parts


def layer_norm(summed, gain_vec, shift_vec):
    centered = summed - jnp.mean(summed, -1, keepdims=True)
    inv_std = lax.rsqrt(jnp.mean(centered * centered, -1, keepdims=True) + EPSILON)
    return centered * inv_std * gain_vec + shift_vec


def matrix_product(left, right):
    return jnp.dot(left, right, preferred_element_type=jnp.float32)


def rows_product(left, right):
    return lax.dot_general(
        left, right, (((0,), (0,)), ((), ())), preferred_element_type=jnp.float32
    )


def back_product(left, right):
    return lax.dot_general(
        left, right, (((1,), (1,)), ((), ())), preferred_element_type=jnp.float32
    )


def feature_map(scaled, directions):
    project = jnp.einsum("rhd,hdm->rhm", scaled, directions, preferred_element_type=jnp.float32)
    widened = scaled.astype(jnp.float32)
    return jnp.exp(project - 0.5 * jnp.sum(widened * widened, -1, keepdims=True))


def feature_back(dfeature, feature, scaled, directions):
    dexponent = dfeature * feature
    dproject = dexponent.astype(jnp.bfloat16)
    dscaled = jnp.einsum("rhm,hdm->rhd", dproject, directions, preferred_element_type=jnp.float32)
    return dscaled - scaled.astype(jnp.float32) * jnp.sum(dexponent, -1, keepdims=True)


def column_sum(values_low):
    return jnp.sum(values_low.astype(jnp.float32), axis=0)


def body(
    tokens,
    cotangent,
    qkv_weight,
    qkv_bias,
    proj_weight,
    proj_bias,
    attn_gain,
    attn_shift,
    inner_weight,
    inner_bias,
    outer_weight,
    outer_bias,
    ffn_gain,
    ffn_shift,
    random_dirs,
    seq_lengths,
    deal_order,
):
    groups = lax.axis_size("fsdp")
    row_count, model_width = tokens.shape
    piece_rows = row_count // groups
    deal_row = deal_order[0]
    send_tokens = jnp.take(tokens.reshape(groups, piece_rows, model_width), deal_row, axis=0)
    send_grads = jnp.take(cotangent.reshape(groups, piece_rows, model_width), deal_row, axis=0)
    replicas = lax.axis_size("replica")
    vectors = (qkv_bias, proj_bias, attn_gain, attn_shift, inner_bias, outer_bias, ffn_gain, ffn_shift)
    sizes = [v.shape[0] for v in vectors]
    small = jnp.broadcast_to(pack_small(vectors, 16)[None], (groups, 16, 128))
    weight_qkv, weight_proj, weight_inner, weight_outer, small_all, arrived_x, arrived_g = gather_all(
        groups, replicas, 0, (qkv_weight, proj_weight, inner_weight, outer_weight), (small, send_tokens, send_grads)
    )
    token_low = arrived_x.reshape(row_count, model_width)
    upstream = arrived_g.reshape(row_count, model_width).astype(jnp.float32)
    bias_qkv, bias_proj, gain_attn, shift_attn, bias_inner, bias_outer, gain_ffn, shift_ffn = (
        v.reshape(-1).astype(jnp.float32) for v in unpack_small(small_all, sizes)
    )
    lengths_here = seq_lengths[0, 0]
    seq_ends = jnp.cumsum(lengths_here)
    slot_count = lengths_here.shape[0] + 1
    position = lax.iota(jnp.int32, row_count)
    segment = jnp.sum((position[:, None] >= seq_ends[None, :]).astype(jnp.int32), axis=1)
    select_low = (segment[:, None] == lax.iota(jnp.int32, slot_count)[None, :]).astype(jnp.bfloat16)
    valid_rows = (segment < slot_count - 1).astype(jnp.float32)[:, None]
    head_count, head_dim = (random_dirs.shape[0], random_dirs.shape[1])
    feature_scale = head_dim ** (-0.25)
    qkv_act = matrix_product(token_low, weight_qkv) + bias_qkv
    query_act, key_act, value_act = jnp.split(qkv_act, 3, axis=1)
    query_low = (
        (query_act * feature_scale).astype(jnp.bfloat16).reshape(row_count, head_count, head_dim)
    )
    key_low = (
        (key_act * feature_scale).astype(jnp.bfloat16).reshape(row_count, head_count, head_dim)
    )
    value_low = value_act.astype(jnp.bfloat16).reshape(row_count, head_count, head_dim)
    query_feat = feature_map(query_low, random_dirs)
    key_feat = feature_map(key_low, random_dirs)
    qfeat_low = query_feat.astype(jnp.bfloat16)
    kfeat_low = key_feat.astype(jnp.bfloat16)
    masked_keys = select_low[:, :, None, None] * kfeat_low[:, None]
    masked_query = select_low[:, :, None, None] * qfeat_low[:, None]
    kv_state = jnp.einsum(
        "rshm,rhe->shme", masked_keys, value_low, preferred_element_type=jnp.float32
    ).astype(jnp.bfloat16)
    key_total = jnp.einsum(
        "rs,rhm->shm", select_low, kfeat_low, preferred_element_type=jnp.float32
    ).astype(jnp.bfloat16)
    numerator = jnp.einsum(
        "rshm,shme->rhe", masked_query, kv_state, preferred_element_type=jnp.float32
    )
    denominator = jnp.einsum(
        "rshm,shm->rh", masked_query, key_total, preferred_element_type=jnp.float32
    )
    context_low = (
        (numerator / denominator[:, :, None]).reshape(row_count, model_width).astype(jnp.bfloat16)
    )
    attn_out = matrix_product(context_low, weight_proj) + bias_proj
    hidden, first_pull = jax.vjp(
        layer_norm, token_low.astype(jnp.float32) + attn_out, gain_attn, shift_attn
    )
    hidden_low = hidden.astype(jnp.bfloat16)
    inner_act = matrix_product(hidden_low, weight_inner) + bias_inner
    gelu_act, gelu_pull = jax.vjp(partial(jax.nn.gelu, approximate=False), inner_act)
    gelu_low = gelu_act.astype(jnp.bfloat16)
    outer_act = matrix_product(gelu_low, weight_outer) + bias_outer
    normed_out, second_pull = jax.vjp(layer_norm, hidden + outer_act, gain_ffn, shift_ffn)
    result = normed_out * valid_rows
    back_qkv, back_proj, back_inner, back_outer = weight_qkv, weight_proj, weight_inner, weight_outer
    dsecond, grad_gain_ffn, grad_shift_ffn = second_pull(upstream * valid_rows)
    douter_low = dsecond.astype(jnp.bfloat16)
    grad_bias_outer = column_sum(douter_low)
    grad_weight_outer = rows_product(gelu_low, douter_low)
    dinner_low = gelu_pull(back_product(douter_low, back_outer))[0].astype(jnp.bfloat16)
    grad_bias_inner = column_sum(dinner_low)
    grad_weight_inner = rows_product(hidden_low, dinner_low)
    dhidden = dsecond + back_product(dinner_low, back_inner)
    dfirst, grad_gain_attn, grad_shift_attn = first_pull(dhidden)
    dattn_low = dfirst.astype(jnp.bfloat16)
    grad_bias_proj = column_sum(dattn_low)
    grad_weight_proj = rows_product(context_low, dattn_low)
    dcontext = back_product(dattn_low, back_proj).reshape(row_count, head_count, head_dim)
    dnumer_low = (dcontext / denominator[:, :, None]).astype(jnp.bfloat16)
    ddenom_low = (-jnp.sum(dcontext * numerator, -1) / jnp.square(denominator)).astype(jnp.bfloat16)
    masked_dnumer = select_low[:, :, None, None] * dnumer_low[:, None]
    key_rows = jnp.einsum("rs,shm->rhm", select_low, key_total, preferred_element_type=jnp.float32)
    dqfeat = jnp.einsum(
        "rshe,shme->rhm", masked_dnumer, kv_state, preferred_element_type=jnp.float32
    )
    dqfeat = dqfeat + ddenom_low.astype(jnp.float32)[:, :, None] * key_rows
    dstate_low = jnp.einsum(
        "rshm,rhe->shme", masked_query, dnumer_low, preferred_element_type=jnp.float32
    ).astype(jnp.bfloat16)
    dtotal_low = jnp.einsum(
        "rshm,rh->shm", masked_query, ddenom_low, preferred_element_type=jnp.float32
    ).astype(jnp.bfloat16)
    masked_values = select_low[:, :, None, None] * value_low[:, None]
    dkfeat = jnp.einsum(
        "rshe,shme->rhm", masked_values, dstate_low, preferred_element_type=jnp.float32
    )
    dkfeat = dkfeat + jnp.einsum(
        "rs,shm->rhm", select_low, dtotal_low, preferred_element_type=jnp.float32
    )
    dvalues = jnp.einsum(
        "rshm,shme->rhe", masked_keys, dstate_low, preferred_element_type=jnp.float32
    )
    dquery = feature_back(dqfeat, query_feat, query_low, random_dirs) * feature_scale
    dkeys = feature_back(dkfeat, key_feat, key_low, random_dirs) * feature_scale
    dqkv_low = jnp.concatenate(
        [
            dquery.reshape(row_count, model_width),
            dkeys.reshape(row_count, model_width),
            dvalues.reshape(row_count, model_width),
        ],
        axis=1,
    ).astype(jnp.bfloat16)
    grad_bias_qkv = column_sum(dqkv_low)
    grad_weight_qkv = rows_product(token_low, dqkv_low)
    dtokens = dfirst + back_product(dqkv_low, back_qkv)
    out_rows = result.astype(jnp.bfloat16).reshape(groups, piece_rows, model_width)
    grad_rows = dtokens.astype(jnp.bfloat16).reshape(groups, piece_rows, model_width)
    vector_grads = (
        grad_bias_qkv,
        grad_bias_proj,
        grad_gain_attn,
        grad_shift_attn,
        grad_bias_inner,
        grad_bias_outer,
        grad_gain_ffn,
        grad_shift_ffn,
    )
    small_grads = pack_small([v.reshape(groups, -1) for v in vector_grads], 8)
    sum_wqkv, sum_wproj, sum_winner, sum_wouter, small_sum, back_out, back_grad = scatter_all(
        groups,
        replicas,
        1,
        [g.astype(jnp.bfloat16) for g in (grad_weight_qkv, grad_weight_proj, grad_weight_inner, grad_weight_outer)],
        small_grads,
        (out_rows, grad_rows),
    )
    sum_bqkv, sum_bproj, sum_gattn, sum_sattn, sum_binner, sum_bouter, sum_gffn, sum_sffn = unpack_small(
        small_sum, sizes
    )
    inverse = jnp.zeros((groups,), jnp.int32).at[deal_row].set(lax.iota(jnp.int32, groups))
    layer_out = jnp.take(back_out, inverse, axis=0).reshape(row_count, model_width)
    tokens_grad = jnp.take(back_grad, inverse, axis=0).reshape(row_count, model_width)
    return (
        layer_out,
        tokens_grad,
        sum_wqkv,
        sum_bqkv,
        sum_wproj,
        sum_bproj,
        sum_gattn,
        sum_sattn,
        sum_winner,
        sum_binner,
        sum_wouter,
        sum_bouter,
        sum_gffn,
        sum_sffn,
    )


def solution(mesh):
    return jax.shard_map(
        body,
        mesh=mesh,
        in_specs=(
            P(("replica", "fsdp"), None),
            P(("replica", "fsdp"), None),
            P("fsdp", None),
            P("fsdp"),
            P("fsdp", None),
            P("fsdp"),
            P("fsdp"),
            P("fsdp"),
            P("fsdp", None),
            P("fsdp"),
            P("fsdp", None),
            P("fsdp"),
            P("fsdp"),
            P("fsdp"),
            P(),
            P("replica", "fsdp", None),
            P("replica", None),
        ),
        out_specs=(
            P(("replica", "fsdp"), None),
            P(("replica", "fsdp"), None),
            P("fsdp", None),
            P("fsdp"),
            P("fsdp", None),
            P("fsdp"),
            P("fsdp"),
            P("fsdp"),
            P("fsdp", None),
            P("fsdp"),
            P("fsdp", None),
            P("fsdp"),
            P("fsdp"),
            P("fsdp"),
        ),
        check_vma=False,
    )
```

```python
from functools import partial

import jax
import jax.numpy as jnp
from jax import lax
from jax.experimental import pallas as pl
from jax.experimental.pallas import tpu as pltpu
from jax.sharding import PartitionSpec as P

EPSILON = 1e-06
ANY = pl.BlockSpec(memory_space=pl.ANY)
VMEM = pl.BlockSpec(memory_space=pltpu.VMEM)
MESH = pl.DeviceIdType.MESH
DMA = pltpu.SemaphoreType.DMA


class Place:
    def __init__(self, n, replicas):
        self.n, self.replicas = n, replicas
        self.nz = 4 if n % 8 == 0 else n // 2
        self.ny = n // (2 * self.nz)
        self.chips = n // 2
        self.f = lax.axis_index("fsdp")
        self.r = lax.axis_index("replica")
        self.core = self.f % 2
        chip = self.f // 2
        y, z = chip % self.ny, chip // self.ny
        odd = y % 2
        self.pos = y * self.nz + z * (1 - odd) + (self.nz - 1 - z) * odd
        self.role = self.r % 2

    def dev(self, pos, core):
        pos = (pos + 2 * self.chips) % self.chips
        y, t = pos // self.nz, pos % self.nz
        odd = y % 2
        z = t * (1 - odd) + (self.nz - 1 - t) * odd
        return (z * self.ny + y) * 2 + core

    def peer(self, f):
        return (self.r, f)

    def ring(self, direction):
        return self.peer(self.dev(self.pos + (1 if direction == 0 else -1), self.core))

    def mate(self):
        return self.peer(self.f + 1 - 2 * self.core)

    def across(self):
        return (self.r + 1 - 2 * self.role, self.f)

    def greet(self):
        barrier = pltpu.get_barrier_semaphore()

        @pl.loop(1, self.n)
        def _(k):
            pl.semaphore_signal(barrier, inc=1, device_id=self.peer((self.f + k) % self.n), device_id_type=MESH)

        @pl.loop(1, self.replicas)
        def _(k):
            pl.semaphore_signal(barrier, inc=1, device_id=((self.r + k) % self.replicas, self.f), device_id_type=MESH)

        pl.semaphore_wait(barrier, self.n - 1 + self.replicas - 1)


def remote(src, dst, send, recv, device):
    return pltpu.make_async_remote_copy(
        src_ref=src, dst_ref=dst, send_sem=send, recv_sem=recv, device_id=device, device_id_type=MESH
    )


class Exchange:
    def __init__(self, place, send, recv, sems):
        self.place, self.send, self.recv = place, send, recv
        self.out_sem, self.in_sem, self.own_sem = sems

    def copy(self, target):
        me = self.place.f
        return remote(
            self.send.at[target], self.recv.at[me], self.out_sem, self.in_sem, self.place.peer(target)
        )

    def own(self):
        me = self.place.f
        return pltpu.make_async_copy(self.send.at[me], self.recv.at[me], self.own_sem)

    def start(self):
        self.own().start()

        @pl.loop(1, self.place.n)
        def _(k):
            self.copy((self.place.f + k) % self.place.n).start()

    def finish(self):
        rest = self.recv.at[pl.ds(0, self.place.n - 1)]
        pltpu.make_async_copy(rest, rest, self.out_sem).wait()
        pltpu.make_async_copy(rest, rest, self.in_sem).wait()
        self.own().wait()


class Gather:
    def __init__(self, place, shard, full, sems):
        self.place, self.shard, self.full = place, shard, full
        self.ring_in, self.across_in, self.flat = sems
        self.rows, self.cols = shard.shape
        split = self.rows % 48 == 0 and place.replicas % 2 == 0
        self.third = self.rows // 3 if split else 0
        self.main = self.rows - self.third
        self.half = self.cols // 2

    def box(self, ref, owner, offset, count, direction):
        row = offset if owner is None else owner * self.rows + offset
        if owner is not None or not isinstance(row, int):
            row = pl.multiple_of(row, 8)
        return ref.at[pl.ds(row, count), pl.ds(direction * self.half, self.half)]

    def origin(self, s, direction):
        return self.place.pos - s if direction == 0 else self.place.pos + s

    def ring_copy(self, s, direction, own=False):
        owner = self.place.dev(self.origin(s, direction), self.place.core)
        lead = self.place.role * self.third
        dst = self.box(self.full, owner, lead, self.main, direction)
        src = self.box(self.shard, None, lead, self.main, direction) if own else dst
        return remote(src, dst, self.flat.at[0], self.ring_in.at[s, direction], self.place.ring(direction))

    def mate_copy(self, s, direction, lead, count):
        owner = self.place.dev(self.origin(s, direction), self.place.core)
        part = self.box(self.full, owner, lead, count, direction)
        return remote(part, part, self.flat.at[1], self.flat.at[2], self.place.mate())

    def across_copy(self, s, direction, arriving=False):
        owner = self.place.dev(self.origin(s, direction), self.place.core)
        role = 1 - self.place.role if arriving else self.place.role
        part = self.box(self.full, owner, role * 2 * self.third, self.third, direction)
        return remote(part, part, self.flat.at[3], self.across_in.at[s - 1, direction], self.place.across())

    def own_copy(self):
        row = pl.multiple_of(self.place.f * self.rows, 8)
        return pltpu.make_async_copy(self.shard, self.full.at[pl.ds(row, self.rows)], self.flat.at[4])

    def start(self):
        for direction in range(2):
            self.ring_copy(0, direction, own=True).start()
        row = pl.multiple_of(self.place.f * self.rows, 8)
        remote(
            self.shard, self.full.at[pl.ds(row, self.rows)], self.flat.at[1], self.flat.at[2], self.place.mate()
        ).start()
        self.own_copy().start()

    def step(self, s, last=False):
        for direction in range(2):
            owner = self.place.dev(self.origin(s, direction), self.place.core)
            lead = self.place.role * self.third
            part = self.box(self.full, owner, lead, self.main, direction)
            remote(part, part, self.flat.at[0], self.ring_in.at[s - 1, direction], self.place.ring(direction)).wait_recv()
            if not last:
                self.ring_copy(s, direction).start()
            if self.third:
                self.across_copy(s, direction).start()
            self.mate_copy(s, direction, lead, self.main).start()

    def across_step(self, s):
        if self.third:
            for direction in range(2):
                self.across_copy(s, direction, arriving=True).wait_recv()
                self.mate_copy(s, direction, (1 - self.place.role) * 2 * self.third, self.third).start()

    def wait_rows(self, count, index):
        part = self.full.at[pl.ds(0, count)]
        pltpu.make_async_copy(part, part, self.flat.at[index]).wait()

    def finish(self):
        hops = self.place.chips - 1
        self.wait_rows(hops * self.main, 0)
        self.wait_rows(self.place.chips * self.rows, 1)
        self.wait_rows(self.place.chips * self.rows, 2)
        if self.third:
            self.wait_rows(hops * self.third, 3)
        self.own_copy().wait()


def gather_kernel(n, replicas, weights, exchanges, *refs):
    refs = list(refs)
    take = lambda count: [refs.pop(0) for _ in range(count)]
    shards, sends = take(weights), take(exchanges)
    fulls, recvs = take(weights), take(exchanges)
    gather_sems = [take(3) for _ in range(weights)]
    exchange_sems = [take(3) for _ in range(exchanges)]
    place = Place(n, replicas)
    gathers = [Gather(place, *item) for item in zip(shards, fulls, gather_sems)]
    swaps = [Exchange(place, *item) for item in zip(sends, recvs, exchange_sems)]
    place.greet()
    for item in gathers:
        item.start()
    for item in swaps:
        item.start()
    hops = place.chips - 1

    for item in gathers:
        item.step(1, last=hops == 1)

    @pl.loop(2, hops)
    def _(s):
        for item in gathers:
            item.step(s)
        for item in gathers:
            item.across_step(s - 1)

    for item in gathers:
        item.step(hops, last=True)
    for item in gathers:
        item.across_step(hops - 1)
    for item in gathers:
        item.across_step(hops)
    for item in gathers:
        item.finish()
    for item in swaps:
        item.finish()


def gather_all(n, replicas, collective_id, shards, sends):
    hops = n // 2 - 1
    outs = [jax.ShapeDtypeStruct((n * a.shape[0], a.shape[1]), a.dtype) for a in shards]
    outs += [jax.ShapeDtypeStruct(a.shape, a.dtype) for a in sends]
    scratch = [DMA((hops, 2)), DMA((hops, 2)), DMA((5,))] * len(shards) + [DMA(()), DMA(()), DMA(())] * len(sends)
    return pl.pallas_call(
        partial(gather_kernel, n, replicas, len(shards), len(sends)),
        out_shape=outs,
        in_specs=[VMEM] * len(shards) + [ANY] * len(sends),
        out_specs=[ANY] * len(outs),
        scratch_shapes=scratch,
        compiler_params=pltpu.CompilerParams(collective_id=collective_id, has_side_effects=True),
        name="gather_all",
    )(*shards, *sends)


class Scatter:
    def __init__(self, place, grad, total, bufs, sems):
        self.place, self.grad, self.total = place, grad, total
        self.own, self.other, self.ringed, self.repl = bufs
        self.own_in, self.core_in, self.ring_in, self.repl_in, self.flat = sems
        self.rows, self.cols = total.shape
        self.half = self.cols // 2

    def rows_of(self, pos, core):
        row = pl.multiple_of(self.place.dev(pos, core) * self.rows, 8)
        return self.grad.at[pl.ds(row, self.rows)]

    def slot(self, pos):
        return (pos + 2 * self.place.chips) % self.place.chips

    def load(self, pos):
        k = self.slot(pos)
        return pltpu.make_async_copy(self.rows_of(pos, self.place.core), self.own.at[k], self.own_in.at[k])

    def give(self, pos):
        k = self.slot(pos)
        return remote(
            self.rows_of(pos, 1 - self.place.core), self.other.at[k], self.flat.at[0], self.core_in.at[k], self.place.mate()
        )

    def start(self):
        def one(k, _):
            pos = self.place.pos + ((k + 2) // 2) * (2 * (k % 2) - 1)
            self.load(pos).start()
            self.give(pos).start()
            return 0

        lax.fori_loop(0, self.place.chips - 1, one, 0)
        self.load(self.place.pos).start()
        self.give(self.place.pos).start()

    def merge(self, pos):
        k = self.slot(pos)
        self.load(pos).wait()
        self.give(pos).wait_recv()
        self.own[k] = (self.own[k].astype(jnp.float32) + self.other[k].astype(jnp.float32)).astype(jnp.bfloat16)

    def target(self, s, direction):
        return self.place.pos - 1 - s if direction == 0 else self.place.pos + 1 + s

    def cols_of(self, direction):
        return pl.ds(direction * self.half, self.half)

    def ring_copy(self, s, direction, first=False):
        cols = self.cols_of(direction)
        if first:
            src = self.own.at[self.slot(self.target(0, direction)), :, cols]
        else:
            src = self.ringed.at[s - 1, :, cols]
        return remote(src, self.ringed.at[s, :, cols], self.flat.at[1], self.ring_in.at[s, direction], self.place.ring(direction))

    def absorb(self, s, direction):
        cols = self.cols_of(direction)
        self.ring_copy(s, direction, first=True).wait_recv()
        k = self.slot(self.target(s + 1, direction))
        self.ringed[s, :, cols] = (
            self.ringed[s, :, cols].astype(jnp.float32) + self.own[k, :, cols].astype(jnp.float32)
        ).astype(jnp.bfloat16)

    def publish(self):
        hops = self.place.chips - 1
        last = self.ringed.at[hops - 1]

        def one(k, _):
            r = (self.place.r + k) % self.place.replicas
            remote(last, self.repl.at[self.place.r], self.flat.at[2], self.repl_in.at[0], (r, self.place.f)).start()
            return 0

        lax.fori_loop(1, self.place.replicas, one, 0)
        self.repl[self.place.r] = self.ringed[hops - 1]

    def finish(self):
        others = self.repl.at[pl.ds(0, self.place.replicas - 1)]
        pltpu.make_async_copy(others, others, self.repl_in.at[0]).wait()
        total = self.repl[0].astype(jnp.float32)
        for r in range(1, self.place.replicas):
            total = total + self.repl[r].astype(jnp.float32)
        self.total[...] = total
        pltpu.make_async_copy(others, others, self.flat.at[2]).wait()
        pltpu.make_async_copy(self.ringed, self.ringed, self.flat.at[1]).wait()
        pltpu.make_async_copy(self.other, self.other, self.flat.at[0]).wait()


def scatter_kernel(n, replicas, weights, exchanges, *refs):
    refs = list(refs)
    take = lambda count: [refs.pop(0) for _ in range(count)]
    grads, (small,), sends = take(weights), take(1), take(exchanges)
    totals, (small_total,), recvs = take(weights), take(1), take(exchanges)
    bufs = [take(4) for _ in range(weights)]
    small_in, small_group = take(2)
    sems = [take(5) for _ in range(weights)]
    small_sems = take(3)
    small_repl, = take(1)
    exchange_sems = [take(3) for _ in range(exchanges)]
    place = Place(n, replicas)
    scatters = [Scatter(place, *item) for item in zip(grads, totals, bufs, sems)]
    swaps = [Exchange(place, *item) for item in zip(sends, recvs, exchange_sems)]
    smalls = Exchange(place, small, small_in, small_sems)
    place.greet()
    hops = place.chips - 1
    for item in scatters:
        item.start()
    smalls.start()
    for item in scatters:
        item.merge(place.pos - 1)
        item.ring_copy(0, 0, first=True).start()
        item.merge(place.pos + 1)
        item.ring_copy(0, 1, first=True).start()
    for item in swaps:
        item.start()
    half = (place.chips - 2) // 2

    def early(s, _):
        for item in scatters:
            item.merge(place.pos - 2 - s)

            @pl.when(s < hops // 2 - 1)
            def _():
                item.merge(place.pos + 2 + s)

            for direction in range(2):
                item.absorb(s, direction)
                item.ring_copy(s + 1, direction).start()
        return 0

    def late(s, _):
        for item in scatters:
            for direction in range(2):
                item.absorb(s, direction)
                item.ring_copy(s + 1, direction).start()
        return 0

    lax.fori_loop(0, half, early, 0)
    lax.fori_loop(half, hops - 1, late, 0)
    smalls.finish()
    group = small_in[0]
    for k in range(1, n):
        group = group + small_in[k]
    small_group[place.r] = group

    def tell(k, _):
        r = (place.r + k) % replicas
        remote(small_group.at[place.r], small_group.at[place.r], small_repl.at[0], small_repl.at[1], (r, place.f)).start()
        return 0

    lax.fori_loop(1, replicas, tell, 0)
    for item in scatters:
        item.merge(place.pos)
        for direction in range(2):
            item.absorb(hops - 1, direction)
        item.publish()
    others = small_group.at[pl.ds(0, replicas - 1)]
    pltpu.make_async_copy(others, others, small_repl.at[1]).wait()
    total = small_group[0]
    for r in range(1, replicas):
        total = total + small_group[r]
    small_total[...] = total
    pltpu.make_async_copy(others, others, small_repl.at[0]).wait()
    for item in scatters:
        item.finish()
    for item in swaps:
        item.finish()


def scatter_all(n, replicas, collective_id, grads, small, sends):
    chips, hops = n // 2, n // 2 - 1
    outs = [jax.ShapeDtypeStruct((a.shape[0] // n, a.shape[1]), jnp.float32) for a in grads]
    outs += [jax.ShapeDtypeStruct(small.shape[1:], jnp.float32)]
    outs += [jax.ShapeDtypeStruct(a.shape, a.dtype) for a in sends]
    scratch = []
    for a in grads:
        block = (a.shape[0] // n, a.shape[1])
        scratch += [pltpu.VMEM((count,) + block, jnp.bfloat16) for count in (chips, chips, hops, replicas)]
    scratch += [pltpu.VMEM(small.shape, jnp.float32), pltpu.VMEM((replicas,) + small.shape[1:], jnp.float32)]
    scratch += [DMA((chips,)), DMA((chips,)), DMA((hops, 2)), DMA((1,)), DMA((3,))] * len(grads)
    scratch += [DMA(()), DMA(()), DMA(()), DMA((2,))] + [DMA(()), DMA(()), DMA(())] * len(sends)
    return pl.pallas_call(
        partial(scatter_kernel, n, replicas, len(grads), len(sends)),
        out_shape=outs,
        in_specs=[ANY] * (len(grads) + 1 + len(sends)),
        out_specs=[VMEM] * (len(grads) + 1) + [ANY] * len(sends),
        scratch_shapes=scratch,
        compiler_params=pltpu.CompilerParams(
            collective_id=collective_id, has_side_effects=True, vmem_limit_bytes=56 << 20
        ),
        name="scatter_all",
    )(*grads, small, *sends)


LANES = 128
SLOTS = 6


def lane_half(shape):
    return lax.broadcasted_iota(jnp.int32, shape, 1) < LANES // 2


def dot_rows(left, right):
    return lax.dot_general(left, right, (((0,), (0,)), ((), ())), preferred_element_type=jnp.float32)


def dot_last(left, right):
    return lax.dot_general(left, right, (((1,), (1,)), ((), ())), preferred_element_type=jnp.float32)


def own_half(wide, head):
    turned = pltpu.roll(wide, LANES // 2, 1)
    first = lane_half(wide.shape)
    return jnp.where(first, wide, turned) if head == 0 else jnp.where(first, turned, wide)


def in_slots(wide, head, mask):
    same = own_half(wide, head).astype(jnp.bfloat16)
    return jnp.concatenate([same] * (SLOTS // 2), axis=1) * mask


def slot_sum(wide, mask):
    picked = wide * mask.astype(jnp.float32)
    both = picked[:, :LANES] + picked[:, LANES : 2 * LANES] + picked[:, 2 * LANES :]
    return both + pltpu.roll(both, LANES // 2, 1)


def half_norm(wide, head):
    keep = lane_half(wide.shape) if head == 0 else jnp.logical_not(lane_half(wide.shape))
    return jnp.sum(jnp.where(keep, wide, 0.0), axis=1, keepdims=True)


def pair_cols(part, pair, width):
    return pl.ds(pl.multiple_of(part * width + pair * LANES, LANES), LANES)


def features(low, directions, head):
    count = directions.shape[1] // 2
    project = jnp.dot(low, directions[:, head * count : (head + 1) * count], preferred_element_type=jnp.float32)
    wide = low.astype(jnp.float32)
    return jnp.exp(project - 0.5 * half_norm(wide * wide, head))


def states(key_low, value_wide, head, mask, segments):
    value_slots = in_slots(value_wide, head, mask)
    state = dot_rows(key_low, value_slots).astype(jnp.bfloat16)
    total = dot_rows(key_low, segments).astype(jnp.bfloat16)
    return value_slots, state, total


def readout(query_low, state, total, mask, segments):
    numer = slot_sum(jnp.dot(query_low, state, preferred_element_type=jnp.float32), mask)
    denom = jnp.dot(query_low, total, preferred_element_type=jnp.float32) * segments.astype(jnp.float32)
    return numer, jnp.sum(denom, axis=1, keepdims=True)


def forward_pair(pair, scale, x_ref, w_ref, b_ref, dirs_ref, mask_ref, seg_ref, qkv_ref, ctx_ref):
    width = x_ref.shape[1]
    rows = x_ref[...]
    parts = []
    for part in range(3):
        cols = pair_cols(part, pair, width)
        act = jnp.dot(rows, w_ref[:, cols], preferred_element_type=jnp.float32) + b_ref[0:1, cols]
        low = (act * scale if part < 2 else act).astype(jnp.bfloat16)
        qkv_ref[:, cols] = low
        parts.append(low)
    query, key, value = parts
    directions = dirs_ref[pair]
    outs = []
    for head in range(2):
        query_low = features(query, directions, head).astype(jnp.bfloat16)
        key_low = features(key, directions, head).astype(jnp.bfloat16)
        _, state, total = states(key_low, value.astype(jnp.float32), head, mask_ref[...], seg_ref[...])
        numer, denom = readout(query_low, state, total, mask_ref[...], seg_ref[...])
        outs.append(numer / denom)
    ctx_ref[:, pair_cols(0, pair, width)] = jnp.where(lane_half(outs[0].shape), outs[0], outs[1]).astype(jnp.bfloat16)


def backward_pair(pair, scale, qkv_ref, dctx_ref, dirs_ref, mask_ref, seg_ref, dqkv_ref):
    width = dctx_ref.shape[1]
    query, key, value = [qkv_ref[:, pair_cols(part, pair, width)] for part in range(3)]
    dctx = dctx_ref[:, pair_cols(0, pair, width)]
    directions = dirs_ref[pair]
    outs = []
    for head in range(2):
        mask, segments = mask_ref[...], seg_ref[...]
        half_dirs = directions[:, head * (directions.shape[1] // 2) : (head + 1) * (directions.shape[1] // 2)]
        query_feat = features(query, directions, head)
        key_feat = features(key, directions, head)
        query_low, key_low = query_feat.astype(jnp.bfloat16), key_feat.astype(jnp.bfloat16)
        value_slots, state, total = states(key_low, value.astype(jnp.float32), head, mask, segments)
        numer, denom = readout(query_low, state, total, mask, segments)
        dnumer_slots = in_slots(dctx / denom, head, mask)
        ddenom = (-half_norm(dctx * numer, head) / (denom * denom)).astype(jnp.bfloat16)
        ddenom_rows = (ddenom.astype(jnp.float32) * segments.astype(jnp.float32)).astype(jnp.bfloat16)
        dquery_feat = dot_last(dnumer_slots, state) + dot_last(ddenom_rows, total)
        dexp = dquery_feat * query_feat
        dquery = dot_last(dexp.astype(jnp.bfloat16), half_dirs) - query.astype(jnp.float32) * jnp.sum(
            dexp, axis=1, keepdims=True
        )
        dstate = dot_rows(query_low, dnumer_slots).astype(jnp.bfloat16)
        dtotal = dot_rows(query_low, ddenom_rows).astype(jnp.bfloat16)
        dkey_feat = dot_last(value_slots, dstate) + dot_last(segments, dtotal)
        dexp = dkey_feat * key_feat
        dkey = dot_last(dexp.astype(jnp.bfloat16), half_dirs) - key.astype(jnp.float32) * jnp.sum(
            dexp, axis=1, keepdims=True
        )
        dvalue = slot_sum(jnp.dot(key_low, dstate, preferred_element_type=jnp.float32), mask)
        outs.append((dquery * scale, dkey * scale, dvalue))
    for part in range(3):
        both = jnp.where(lane_half(outs[0][part].shape), outs[0][part], outs[1][part])
        dqkv_ref[:, pair_cols(part, pair, width)] = both.astype(jnp.bfloat16)


def forward_kernel(pairs, scale, *refs):
    @pl.loop(0, pairs)
    def _(pair):
        forward_pair(pair, scale, *refs)


def backward_kernel(pairs, scale, *refs):
    @pl.loop(0, pairs)
    def _(pair):
        backward_pair(pair, scale, *refs)


def attend(pairs, scale, tokens, weight, bias, dirs, mask, segments):
    rows, width = tokens.shape
    outs = [jax.ShapeDtypeStruct((rows, 3 * width), jnp.bfloat16), jax.ShapeDtypeStruct((rows, width), jnp.bfloat16)]
    return pl.pallas_call(
        partial(forward_kernel, pairs, scale),
        out_shape=outs,
        in_specs=[VMEM] * 6,
        out_specs=[VMEM] * 2,
        compiler_params=pltpu.CompilerParams(vmem_limit_bytes=56 << 20),
        name="attend",
    )(tokens, weight, bias, dirs, mask, segments)


def attend_back(pairs, scale, qkv, dcontext, dirs, mask, segments):
    return pl.pallas_call(
        partial(backward_kernel, pairs, scale),
        out_shape=jax.ShapeDtypeStruct(qkv.shape, jnp.bfloat16),
        in_specs=[VMEM] * 5,
        out_specs=VMEM,
        compiler_params=pltpu.CompilerParams(vmem_limit_bytes=56 << 20),
        name="attend_back",
    )(qkv, dcontext, dirs, mask, segments)


def pair_directions(directions):
    heads, size, count = directions.shape
    paired = directions.reshape(heads // 2, 2, size, count)
    zero = jnp.zeros_like(paired[:, 0])
    top = jnp.concatenate([paired[:, 0], zero], axis=2)
    low = jnp.concatenate([zero, paired[:, 1]], axis=2)
    return jnp.concatenate([top, low], axis=1)


def pack_small(vectors, rows):
    joined = jnp.concatenate(vectors, axis=-1)
    room = rows * 128 - joined.shape[-1]
    joined = jnp.pad(joined, [(0, 0)] * (joined.ndim - 1) + [(0, room)])
    return joined.reshape(joined.shape[:-1] + (rows, 128))


def unpack_small(packed, sizes):
    flat = packed.reshape(packed.shape[:-2] + (-1,))
    parts, at = [], 0
    for size in sizes:
        parts.append(flat[..., at : at + size])
        at += size
    return parts


def layer_norm(summed, gain_vec, shift_vec):
    centered = summed - jnp.mean(summed, -1, keepdims=True)
    inv_std = lax.rsqrt(jnp.mean(centered * centered, -1, keepdims=True) + EPSILON)
    return centered * inv_std * gain_vec + shift_vec


def matrix_product(left, right):
    return jnp.dot(left, right, preferred_element_type=jnp.float32)


def rows_product(left, right):
    return lax.dot_general(
        left, right, (((0,), (0,)), ((), ())), preferred_element_type=jnp.float32
    )


def back_product(left, right):
    return lax.dot_general(
        left, right, (((1,), (1,)), ((), ())), preferred_element_type=jnp.float32
    )


def column_sum(values_low):
    return jnp.sum(values_low.astype(jnp.float32), axis=0)


def body(
    tokens,
    cotangent,
    qkv_weight,
    qkv_bias,
    proj_weight,
    proj_bias,
    attn_gain,
    attn_shift,
    inner_weight,
    inner_bias,
    outer_weight,
    outer_bias,
    ffn_gain,
    ffn_shift,
    random_dirs,
    seq_lengths,
    deal_order,
):
    groups = lax.axis_size("fsdp")
    row_count, model_width = tokens.shape
    piece_rows = row_count // groups
    deal_row = deal_order[0]
    send_tokens = jnp.take(tokens.reshape(groups, piece_rows, model_width), deal_row, axis=0)
    send_grads = jnp.take(cotangent.reshape(groups, piece_rows, model_width), deal_row, axis=0)
    replicas = lax.axis_size("replica")
    vectors = (qkv_bias, proj_bias, attn_gain, attn_shift, inner_bias, outer_bias, ffn_gain, ffn_shift)
    sizes = [v.shape[0] for v in vectors]
    small = jnp.broadcast_to(pack_small(vectors, 16)[None], (groups, 16, 128))
    weight_qkv, weight_proj, weight_inner, weight_outer, small_all, arrived_x, arrived_g = gather_all(
        groups, replicas, 0, (qkv_weight, proj_weight, inner_weight, outer_weight), (small, send_tokens, send_grads)
    )
    token_low = arrived_x.reshape(row_count, model_width)
    upstream = arrived_g.reshape(row_count, model_width).astype(jnp.float32)
    bias_qkv, bias_proj, gain_attn, shift_attn, bias_inner, bias_outer, gain_ffn, shift_ffn = (
        v.reshape(-1).astype(jnp.float32) for v in unpack_small(small_all, sizes)
    )
    lengths_here = seq_lengths[0, 0]
    seq_ends = jnp.cumsum(lengths_here)
    slot_count = lengths_here.shape[0] + 1
    position = lax.iota(jnp.int32, row_count)
    segment = jnp.sum((position[:, None] >= seq_ends[None, :]).astype(jnp.int32), axis=1)
    slot_of = lax.iota(jnp.int32, SLOTS * LANES // 2) // (LANES // 2)
    slot_mask = (segment[:, None] == slot_of[None, :]).astype(jnp.bfloat16)
    segments = (segment[:, None] == lax.iota(jnp.int32, LANES)[None, :]).astype(jnp.bfloat16)
    directions = pair_directions(random_dirs)
    valid_rows = (segment < slot_count - 1).astype(jnp.float32)[:, None]
    head_count, head_dim = (random_dirs.shape[0], random_dirs.shape[1])
    feature_scale = head_dim ** (-0.25)
    pairs = head_count // 2
    qkv_low, context_low = attend(
        pairs, feature_scale, token_low, weight_qkv, bias_qkv[None], directions, slot_mask, segments
    )
    attn_out = matrix_product(context_low, weight_proj) + bias_proj
    hidden, first_pull = jax.vjp(
        layer_norm, token_low.astype(jnp.float32) + attn_out, gain_attn, shift_attn
    )
    hidden_low = hidden.astype(jnp.bfloat16)
    inner_act = matrix_product(hidden_low, weight_inner) + bias_inner
    gelu_act, gelu_pull = jax.vjp(partial(jax.nn.gelu, approximate=False), inner_act)
    gelu_low = gelu_act.astype(jnp.bfloat16)
    outer_act = matrix_product(gelu_low, weight_outer) + bias_outer
    normed_out, second_pull = jax.vjp(layer_norm, hidden + outer_act, gain_ffn, shift_ffn)
    result = normed_out * valid_rows
    back_qkv, back_proj, back_inner, back_outer = weight_qkv, weight_proj, weight_inner, weight_outer
    dsecond, grad_gain_ffn, grad_shift_ffn = second_pull(upstream * valid_rows)
    douter_low = dsecond.astype(jnp.bfloat16)
    grad_bias_outer = column_sum(douter_low)
    grad_weight_outer = rows_product(gelu_low, douter_low)
    dinner_low = gelu_pull(back_product(douter_low, back_outer))[0].astype(jnp.bfloat16)
    grad_bias_inner = column_sum(dinner_low)
    grad_weight_inner = rows_product(hidden_low, dinner_low)
    dhidden = dsecond + back_product(dinner_low, back_inner)
    dfirst, grad_gain_attn, grad_shift_attn = first_pull(dhidden)
    dattn_low = dfirst.astype(jnp.bfloat16)
    grad_bias_proj = column_sum(dattn_low)
    grad_weight_proj = rows_product(context_low, dattn_low)
    dcontext = back_product(dattn_low, back_proj)
    dqkv_low = attend_back(pairs, feature_scale, qkv_low, dcontext, directions, slot_mask, segments)
    grad_bias_qkv = column_sum(dqkv_low)
    grad_weight_qkv = rows_product(token_low, dqkv_low)
    dtokens = dfirst + back_product(dqkv_low, back_qkv)
    out_rows = result.astype(jnp.bfloat16).reshape(groups, piece_rows, model_width)
    grad_rows = dtokens.astype(jnp.bfloat16).reshape(groups, piece_rows, model_width)
    vector_grads = (
        grad_bias_qkv,
        grad_bias_proj,
        grad_gain_attn,
        grad_shift_attn,
        grad_bias_inner,
        grad_bias_outer,
        grad_gain_ffn,
        grad_shift_ffn,
    )
    small_grads = pack_small([v.reshape(groups, -1) for v in vector_grads], 8)
    sum_wqkv, sum_wproj, sum_winner, sum_wouter, small_sum, back_out, back_grad = scatter_all(
        groups,
        replicas,
        1,
        [g.astype(jnp.bfloat16) for g in (grad_weight_qkv, grad_weight_proj, grad_weight_inner, grad_weight_outer)],
        small_grads,
        (out_rows, grad_rows),
    )
    sum_bqkv, sum_bproj, sum_gattn, sum_sattn, sum_binner, sum_bouter, sum_gffn, sum_sffn = unpack_small(
        small_sum, sizes
    )
    inverse = jnp.zeros((groups,), jnp.int32).at[deal_row].set(lax.iota(jnp.int32, groups))
    layer_out = jnp.take(back_out, inverse, axis=0).reshape(row_count, model_width)
    tokens_grad = jnp.take(back_grad, inverse, axis=0).reshape(row_count, model_width)
    return (
        layer_out,
        tokens_grad,
        sum_wqkv,
        sum_bqkv,
        sum_wproj,
        sum_bproj,
        sum_gattn,
        sum_sattn,
        sum_winner,
        sum_binner,
        sum_wouter,
        sum_bouter,
        sum_gffn,
        sum_sffn,
    )


def solution(mesh):
    return jax.shard_map(
        body,
        mesh=mesh,
        in_specs=(
            P(("replica", "fsdp"), None),
            P(("replica", "fsdp"), None),
            P("fsdp", None),
            P("fsdp"),
            P("fsdp", None),
            P("fsdp"),
            P("fsdp"),
            P("fsdp"),
            P("fsdp", None),
            P("fsdp"),
            P("fsdp", None),
            P("fsdp"),
            P("fsdp"),
            P("fsdp"),
            P(),
            P("replica", "fsdp", None),
            P("replica", None),
        ),
        out_specs=(
            P(("replica", "fsdp"), None),
            P(("replica", "fsdp"), None),
            P("fsdp", None),
            P("fsdp"),
            P("fsdp", None),
            P("fsdp"),
            P("fsdp"),
            P("fsdp"),
            P("fsdp", None),
            P("fsdp"),
            P("fsdp", None),
            P("fsdp"),
            P("fsdp"),
            P("fsdp"),
        ),
        check_vma=False,
    )
```

```python
from functools import partial

import jax
import jax.numpy as jnp
from jax import lax
from jax.experimental import pallas as pl
from jax.experimental.pallas import tpu as pltpu
from jax.sharding import PartitionSpec as P

EPSILON = 1e-06
ANY = pl.BlockSpec(memory_space=pl.ANY)
VMEM = pl.BlockSpec(memory_space=pltpu.VMEM)
MESH = pl.DeviceIdType.MESH
DMA = pltpu.SemaphoreType.DMA


class Place:
    def __init__(self, n, replicas):
        self.n, self.replicas = n, replicas
        self.nz = 4 if n % 8 == 0 else n // 2
        self.ny = n // (2 * self.nz)
        self.chips = n // 2
        self.f = lax.axis_index("fsdp")
        self.r = lax.axis_index("replica")
        self.core = self.f % 2
        chip = self.f // 2
        y, z = chip % self.ny, chip // self.ny
        odd = y % 2
        self.pos = y * self.nz + z * (1 - odd) + (self.nz - 1 - z) * odd
        self.role = self.r % 2

    def dev(self, pos, core):
        pos = (pos + 2 * self.chips) % self.chips
        y, t = pos // self.nz, pos % self.nz
        odd = y % 2
        z = t * (1 - odd) + (self.nz - 1 - t) * odd
        return (z * self.ny + y) * 2 + core

    def peer(self, f):
        return (self.r, f)

    def ring(self, direction):
        return self.peer(self.dev(self.pos + (1 if direction == 0 else -1), self.core))

    def mate(self):
        return self.peer(self.f + 1 - 2 * self.core)

    def across(self):
        return (self.r + 1 - 2 * self.role, self.f)

    def greet(self):
        barrier = pltpu.get_barrier_semaphore()

        @pl.loop(1, self.n)
        def _(k):
            pl.semaphore_signal(barrier, inc=1, device_id=self.peer((self.f + k) % self.n), device_id_type=MESH)

        @pl.loop(1, self.replicas)
        def _(k):
            pl.semaphore_signal(barrier, inc=1, device_id=((self.r + k) % self.replicas, self.f), device_id_type=MESH)

        pl.semaphore_wait(barrier, self.n - 1 + self.replicas - 1)


def remote(src, dst, send, recv, device):
    return pltpu.make_async_remote_copy(
        src_ref=src, dst_ref=dst, send_sem=send, recv_sem=recv, device_id=device, device_id_type=MESH
    )


class Exchange:
    def __init__(self, place, send, recv, sems):
        self.place, self.send, self.recv = place, send, recv
        self.out_sem, self.in_sem, self.own_sem = sems

    def copy(self, target):
        me = self.place.f
        return remote(
            self.send.at[target], self.recv.at[me], self.out_sem, self.in_sem, self.place.peer(target)
        )

    def own(self):
        me = self.place.f
        return pltpu.make_async_copy(self.send.at[me], self.recv.at[me], self.own_sem)

    def start(self):
        self.own().start()

        @pl.loop(1, self.place.n)
        def _(k):
            self.copy((self.place.f + k) % self.place.n).start()

    def finish(self):
        rest = self.recv.at[pl.ds(0, self.place.n - 1)]
        pltpu.make_async_copy(rest, rest, self.out_sem).wait()
        pltpu.make_async_copy(rest, rest, self.in_sem).wait()
        self.own().wait()


class Spread(Exchange):
    def copy(self, target):
        return remote(
            self.send, self.recv.at[self.place.f], self.out_sem, self.in_sem, self.place.peer(target)
        )

    def own(self):
        return pltpu.make_async_copy(self.send, self.recv.at[self.place.f], self.own_sem)


class Gather:
    def __init__(self, place, shard, full, sems):
        self.place, self.shard, self.full = place, shard, full
        self.ring_in, self.across_in, self.flat = sems
        self.rows, self.cols = shard.shape
        split = self.rows % 48 == 0 and place.replicas % 2 == 0
        self.third = self.rows // 3 if split else 0
        self.main = self.rows - self.third
        self.half = self.cols // 2

    def box(self, ref, owner, offset, count, direction):
        row = offset if owner is None else owner * self.rows + offset
        if owner is not None or not isinstance(row, int):
            row = pl.multiple_of(row, 8)
        return ref.at[pl.ds(row, count), pl.ds(direction * self.half, self.half)]

    def origin(self, s, direction):
        return self.place.pos - s if direction == 0 else self.place.pos + s

    def ring_copy(self, s, direction, own=False):
        owner = self.place.dev(self.origin(s, direction), self.place.core)
        lead = self.place.role * self.third
        dst = self.box(self.full, owner, lead, self.main, direction)
        src = self.box(self.shard, None, lead, self.main, direction) if own else dst
        return remote(src, dst, self.flat.at[0], self.ring_in.at[s, direction], self.place.ring(direction))

    def mate_copy(self, s, direction, lead, count):
        owner = self.place.dev(self.origin(s, direction), self.place.core)
        part = self.box(self.full, owner, lead, count, direction)
        return remote(part, part, self.flat.at[1], self.flat.at[2], self.place.mate())

    def across_copy(self, s, direction, arriving=False):
        owner = self.place.dev(self.origin(s, direction), self.place.core)
        role = 1 - self.place.role if arriving else self.place.role
        part = self.box(self.full, owner, role * 2 * self.third, self.third, direction)
        return remote(part, part, self.flat.at[3], self.across_in.at[s - 1, direction], self.place.across())

    def own_copy(self):
        row = pl.multiple_of(self.place.f * self.rows, 8)
        return pltpu.make_async_copy(self.shard, self.full.at[pl.ds(row, self.rows)], self.flat.at[4])

    def start(self):
        for direction in range(2):
            self.ring_copy(0, direction, own=True).start()
        row = pl.multiple_of(self.place.f * self.rows, 8)
        remote(
            self.shard, self.full.at[pl.ds(row, self.rows)], self.flat.at[1], self.flat.at[2], self.place.mate()
        ).start()
        self.own_copy().start()

    def step(self, s, last=False):
        for direction in range(2):
            owner = self.place.dev(self.origin(s, direction), self.place.core)
            lead = self.place.role * self.third
            part = self.box(self.full, owner, lead, self.main, direction)
            remote(part, part, self.flat.at[0], self.ring_in.at[s - 1, direction], self.place.ring(direction)).wait_recv()
            if not last:
                self.ring_copy(s, direction).start()
            if self.third:
                self.across_copy(s, direction).start()
            self.mate_copy(s, direction, lead, self.main).start()

    def across_step(self, s):
        if self.third:
            for direction in range(2):
                self.across_copy(s, direction, arriving=True).wait_recv()
                self.mate_copy(s, direction, (1 - self.place.role) * 2 * self.third, self.third).start()

    def wait_rows(self, count, index):
        part = self.full.at[pl.ds(0, count)]
        pltpu.make_async_copy(part, part, self.flat.at[index]).wait()

    def finish(self):
        hops = self.place.chips - 1
        self.wait_rows(hops * self.main, 0)
        self.wait_rows(self.place.chips * self.rows, 1)
        self.wait_rows(self.place.chips * self.rows, 2)
        if self.third:
            self.wait_rows(hops * self.third, 3)
        self.own_copy().wait()


class Work:
    def __init__(self, body=None, count=0, ins=(), outs=()):
        self.body, self.count, self.ins, self.outs = body, count, tuple(ins), tuple(outs)

    def at(self, index, refs):
        if self.count:

            @pl.when(index < self.count)
            def _():
                self.body(index, *refs)

    def rest(self, start, refs):
        if self.count > start:

            @pl.loop(start, self.count)
            def _(index):
                self.body(index, *refs)


def gather_kernel(n, replicas, weights, vectors, exchanges, work, *refs):
    refs = list(refs)
    take = lambda count: [refs.pop(0) for _ in range(count)]
    spreads = 1 if vectors else 0
    shards, singles, sends, ins = take(weights), take(vectors), take(exchanges), take(len(work.ins))
    fulls, spread_outs, recvs, outs = take(weights), take(spreads), take(exchanges), take(len(work.outs))
    packed = take(spreads)
    gather_sems = [take(3) for _ in range(weights)]
    spread_sems = [take(3) for _ in range(spreads)]
    exchange_sems = [take(3) for _ in range(exchanges)]
    place = Place(n, replicas)
    gathers = [Gather(place, *item) for item in zip(shards, fulls, gather_sems)]
    swaps = [Spread(place, *item) for item in zip(packed, spread_outs, spread_sems)]
    swaps += [Exchange(place, *item) for item in zip(sends, recvs, exchange_sems)]
    for row, single in enumerate(singles):
        packed[0][row : row + 1, : single.shape[1]] = single[...].astype(jnp.float32)
    place.greet()
    for item in gathers:
        item.start()
    for item in swaps:
        item.start()
    hops = place.chips - 1

    @pl.loop(1, hops)
    def _(s):
        work.at(s - 1, ins + outs)
        for item in gathers:
            item.step(s)

        @pl.when(s > 1)
        def _():
            for item in gathers:
                item.across_step(s - 1)

    for item in gathers:
        item.step(hops, last=True)
    for item in gathers:
        item.across_step(hops - 1)
    for item in gathers:
        item.across_step(hops)
    work.rest(hops - 1, ins + outs)
    for item in gathers:
        item.finish()
    for item in swaps:
        item.finish()


def gather_all(n, replicas, collective_id, shards, singles, sends, work=Work()):
    hops = n // 2 - 1
    outs = [jax.ShapeDtypeStruct((n * a.shape[0], a.shape[1]), a.dtype) for a in shards]
    scratch = []
    block = (8, 256)
    if singles:
        outs += [jax.ShapeDtypeStruct((n,) + block, jnp.float32)]
        scratch += [pltpu.VMEM(block, jnp.float32)]
    outs += [jax.ShapeDtypeStruct(a.shape, a.dtype) for a in sends]
    scratch += [DMA((hops, 2)), DMA((hops, 2)), DMA((5,))] * len(shards)
    scratch += [DMA(()), DMA(()), DMA(())] * (len(sends) + (1 if singles else 0))
    return pl.pallas_call(
        partial(gather_kernel, n, replicas, len(shards), len(singles), len(sends), work),
        out_shape=outs + list(work.outs),
        in_specs=[VMEM] * (len(shards) + len(singles)) + [ANY] * len(sends) + [VMEM] * len(work.ins),
        out_specs=[ANY] * len(outs) + [VMEM] * len(work.outs),
        scratch_shapes=scratch,
        compiler_params=pltpu.CompilerParams(
            collective_id=collective_id, has_side_effects=True, vmem_limit_bytes=56 << 20
        ),
        name="gather_all",
    )(*shards, *singles, *sends, *work.ins)


class Scatter:
    def __init__(self, place, grad, total, bufs, sems):
        self.place, self.grad, self.total = place, grad, total
        self.own, self.other, self.ringed, self.repl = bufs
        self.own_in, self.core_in, self.ring_in, self.repl_in, self.flat = sems
        self.rows, self.cols = total.shape
        self.half = self.cols // 2

    def rows_of(self, pos, core):
        row = pl.multiple_of(self.place.dev(pos, core) * self.rows, 8)
        return self.grad.at[pl.ds(row, self.rows)]

    def slot(self, pos):
        return (pos + 2 * self.place.chips) % self.place.chips

    def load(self, pos):
        k = self.slot(pos)
        return pltpu.make_async_copy(self.rows_of(pos, self.place.core), self.own.at[k], self.own_in.at[k])

    def give(self, pos):
        k = self.slot(pos)
        return remote(
            self.rows_of(pos, 1 - self.place.core), self.other.at[k], self.flat.at[0], self.core_in.at[k], self.place.mate()
        )

    def start(self):
        def one(k, _):
            pos = self.place.pos + ((k + 2) // 2) * (2 * (k % 2) - 1)
            self.load(pos).start()
            self.give(pos).start()
            return 0

        lax.fori_loop(0, self.place.chips - 1, one, 0)
        self.load(self.place.pos).start()
        self.give(self.place.pos).start()

    def merge(self, pos):
        k = self.slot(pos)
        self.load(pos).wait()
        self.give(pos).wait_recv()
        self.own[k] = (self.own[k].astype(jnp.float32) + self.other[k].astype(jnp.float32)).astype(jnp.bfloat16)

    def target(self, s, direction):
        return self.place.pos - 1 - s if direction == 0 else self.place.pos + 1 + s

    def cols_of(self, direction):
        return pl.ds(direction * self.half, self.half)

    def ring_copy(self, s, direction, first=False):
        cols = self.cols_of(direction)
        if first:
            src = self.own.at[self.slot(self.target(0, direction)), :, cols]
        else:
            src = self.ringed.at[s - 1, :, cols]
        return remote(src, self.ringed.at[s, :, cols], self.flat.at[1], self.ring_in.at[s, direction], self.place.ring(direction))

    def absorb(self, s, direction):
        cols = self.cols_of(direction)
        self.ring_copy(s, direction, first=True).wait_recv()
        k = self.slot(self.target(s + 1, direction))
        self.ringed[s, :, cols] = (
            self.ringed[s, :, cols].astype(jnp.float32) + self.own[k, :, cols].astype(jnp.float32)
        ).astype(jnp.bfloat16)

    def publish(self):
        hops = self.place.chips - 1
        last = self.ringed.at[hops - 1]

        def one(k, _):
            r = (self.place.r + k) % self.place.replicas
            remote(last, self.repl.at[self.place.r], self.flat.at[2], self.repl_in.at[0], (r, self.place.f)).start()
            return 0

        lax.fori_loop(1, self.place.replicas, one, 0)
        self.repl[self.place.r] = self.ringed[hops - 1]

    def finish(self):
        others = self.repl.at[pl.ds(0, self.place.replicas - 1)]
        pltpu.make_async_copy(others, others, self.repl_in.at[0]).wait()
        total = self.repl[0].astype(jnp.float32)
        for r in range(1, self.place.replicas):
            total = total + self.repl[r].astype(jnp.float32)
        self.total[...] = total
        pltpu.make_async_copy(others, others, self.flat.at[2]).wait()
        pltpu.make_async_copy(self.ringed, self.ringed, self.flat.at[1]).wait()
        pltpu.make_async_copy(self.other, self.other, self.flat.at[0]).wait()


def scatter_kernel(n, replicas, weights, spreads, exchanges, work, *refs):
    refs = list(refs)
    take = lambda count: [refs.pop(0) for _ in range(count)]
    grads, small, sends, ins = take(weights), take(spreads), take(exchanges), take(len(work.ins))
    totals, small_total, recvs, outs = take(weights), take(spreads), take(exchanges), take(len(work.outs))
    bufs = [take(4) for _ in range(weights)]
    small_bufs = take(2 * spreads)
    sems = [take(5) for _ in range(weights)]
    small_sems = take(4 * spreads)
    exchange_sems = [take(3) for _ in range(exchanges)]
    place = Place(n, replicas)
    scatters = [Scatter(place, *item) for item in zip(grads, totals, bufs, sems)]
    swaps = [Exchange(place, *item) for item in zip(sends, recvs, exchange_sems)]
    place.greet()
    hops = place.chips - 1
    for item in scatters:
        item.start()
    if spreads:
        small_in, small_group = small_bufs
        small_repl = small_sems[3]
        smalls = Exchange(place, small[0], small_in, small_sems[:3])
        smalls.start()
    for item in scatters:
        item.merge(place.pos - 1)
        item.ring_copy(0, 0, first=True).start()
        item.merge(place.pos + 1)
        item.ring_copy(0, 1, first=True).start()
    for item in swaps:
        item.start()

    @pl.loop(0, hops - 1)
    def _(s):
        work.at(s, ins + outs)
        for item in scatters:

            @pl.when(s < (place.chips - 2) // 2)
            def _():
                item.merge(place.pos - 2 - s)

            @pl.when(s < hops // 2 - 1)
            def _():
                item.merge(place.pos + 2 + s)

            for direction in range(2):
                item.absorb(s, direction)
                item.ring_copy(s + 1, direction).start()

    work.rest(hops - 1, ins + outs)
    if spreads:
        smalls.finish()
        group = small_in[0]
        for k in range(1, n):
            group = group + small_in[k]
        small_group[place.r] = group

        @pl.loop(1, replicas)
        def _(k):
            mine = small_group.at[place.r]
            target = ((place.r + k) % replicas, place.f)
            remote(mine, mine, small_repl.at[0], small_repl.at[1], target).start()

    for item in scatters:
        item.merge(place.pos)
        for direction in range(2):
            item.absorb(hops - 1, direction)
        item.publish()
    if spreads:
        others = small_group.at[pl.ds(0, replicas - 1)]
        pltpu.make_async_copy(others, others, small_repl.at[1]).wait()
        total = small_group[0]
        for r in range(1, replicas):
            total = total + small_group[r]
        small_total[0][...] = total
        pltpu.make_async_copy(others, others, small_repl.at[0]).wait()
    for item in scatters:
        item.finish()
    for item in swaps:
        item.finish()


def scatter_all(n, replicas, collective_id, grads, small, sends, work=Work()):
    chips, hops = n // 2, n // 2 - 1
    outs = [jax.ShapeDtypeStruct((a.shape[0] // n, a.shape[1]), jnp.float32) for a in grads]
    outs += [jax.ShapeDtypeStruct(a.shape[1:], jnp.float32) for a in small]
    wide = [jax.ShapeDtypeStruct(a.shape, a.dtype) for a in sends]
    scratch = []
    for a in grads:
        block = (a.shape[0] // n, a.shape[1])
        scratch += [pltpu.VMEM((count,) + block, jnp.bfloat16) for count in (chips, chips, hops, replicas)]
    for a in small:
        scratch += [pltpu.VMEM(a.shape, jnp.float32), pltpu.VMEM((replicas,) + a.shape[1:], jnp.float32)]
    scratch += [DMA((chips,)), DMA((chips,)), DMA((hops, 2)), DMA((1,)), DMA((3,))] * len(grads)
    scratch += [DMA(()), DMA(()), DMA(()), DMA((2,))] * len(small) + [DMA(()), DMA(()), DMA(())] * len(sends)
    return pl.pallas_call(
        partial(scatter_kernel, n, replicas, len(grads), len(small), len(sends), work),
        out_shape=outs + wide + list(work.outs),
        in_specs=[ANY] * (len(grads) + len(small) + len(sends)) + [VMEM] * len(work.ins),
        out_specs=[VMEM] * len(outs) + [ANY] * len(wide) + [VMEM] * len(work.outs),
        scratch_shapes=scratch,
        compiler_params=pltpu.CompilerParams(
            collective_id=collective_id, has_side_effects=True, vmem_limit_bytes=56 << 20
        ),
        name="scatter_all",
    )(*grads, *small, *sends, *work.ins)


LANES = 128
SLOTS = 6


def lane_half(shape):
    return lax.broadcasted_iota(jnp.int32, shape, 1) < LANES // 2


def dot_rows(left, right):
    return lax.dot_general(left, right, (((0,), (0,)), ((), ())), preferred_element_type=jnp.float32)


def dot_last(left, right):
    return lax.dot_general(left, right, (((1,), (1,)), ((), ())), preferred_element_type=jnp.float32)


def own_half(wide, head):
    turned = pltpu.roll(wide, LANES // 2, 1)
    first = lane_half(wide.shape)
    return jnp.where(first, wide, turned) if head == 0 else jnp.where(first, turned, wide)


def in_slots(wide, head, mask):
    same = own_half(wide, head).astype(jnp.bfloat16)
    return jnp.concatenate([same] * (SLOTS // 2), axis=1) * mask


def slot_sum(wide, mask):
    picked = wide * mask.astype(jnp.float32)
    both = picked[:, :LANES] + picked[:, LANES : 2 * LANES] + picked[:, 2 * LANES :]
    return both + pltpu.roll(both, LANES // 2, 1)


def half_norm(wide, head):
    keep = lane_half(wide.shape) if head == 0 else jnp.logical_not(lane_half(wide.shape))
    return jnp.sum(jnp.where(keep, wide, 0.0), axis=1, keepdims=True)


def pair_cols(part, pair, width):
    return pl.ds(pl.multiple_of(part * width + pair * LANES, LANES), LANES)


def features(low, directions, head):
    count = directions.shape[1] // 2
    project = jnp.dot(low, directions[:, head * count : (head + 1) * count], preferred_element_type=jnp.float32)
    wide = low.astype(jnp.float32)
    return jnp.exp(project - 0.5 * half_norm(wide * wide, head))


def states(key_low, value_wide, head, mask, segments):
    value_slots = in_slots(value_wide, head, mask)
    state = dot_rows(key_low, value_slots).astype(jnp.bfloat16)
    total = dot_rows(key_low, segments).astype(jnp.bfloat16)
    return value_slots, state, total


def readout(query_low, state, total, mask, segments):
    numer = slot_sum(jnp.dot(query_low, state, preferred_element_type=jnp.float32), mask)
    denom = jnp.dot(query_low, total, preferred_element_type=jnp.float32) * segments.astype(jnp.float32)
    return numer, jnp.sum(denom, axis=1, keepdims=True)


def forward_pair(pair, scale, x_ref, w_ref, b_ref, dirs_ref, mask_ref, seg_ref, qkv_ref, ctx_ref):
    width = x_ref.shape[1]
    rows = x_ref[...]
    parts = []
    for part in range(3):
        cols = pair_cols(part, pair, width)
        act = jnp.dot(rows, w_ref[:, cols], preferred_element_type=jnp.float32) + b_ref[0:1, cols]
        low = (act * scale if part < 2 else act).astype(jnp.bfloat16)
        qkv_ref[:, cols] = low
        parts.append(low)
    query, key, value = parts
    directions = dirs_ref[pair]
    outs = []
    for head in range(2):
        query_low = features(query, directions, head).astype(jnp.bfloat16)
        key_low = features(key, directions, head).astype(jnp.bfloat16)
        _, state, total = states(key_low, value.astype(jnp.float32), head, mask_ref[...], seg_ref[...])
        numer, denom = readout(query_low, state, total, mask_ref[...], seg_ref[...])
        outs.append(numer / denom)
    ctx_ref[:, pair_cols(0, pair, width)] = jnp.where(lane_half(outs[0].shape), outs[0], outs[1]).astype(jnp.bfloat16)


def backward_pair(pair, scale, qkv_ref, dctx_ref, dirs_ref, mask_ref, seg_ref, dqkv_ref):
    width = dctx_ref.shape[1]
    query, key, value = [qkv_ref[:, pair_cols(part, pair, width)] for part in range(3)]
    dctx = dctx_ref[:, pair_cols(0, pair, width)]
    directions = dirs_ref[pair]
    outs = []
    for head in range(2):
        mask, segments = mask_ref[...], seg_ref[...]
        half_dirs = directions[:, head * (directions.shape[1] // 2) : (head + 1) * (directions.shape[1] // 2)]
        query_feat = features(query, directions, head)
        key_feat = features(key, directions, head)
        query_low, key_low = query_feat.astype(jnp.bfloat16), key_feat.astype(jnp.bfloat16)
        value_slots, state, total = states(key_low, value.astype(jnp.float32), head, mask, segments)
        numer, denom = readout(query_low, state, total, mask, segments)
        dnumer_slots = in_slots(dctx / denom, head, mask)
        ddenom = (-half_norm(dctx * numer, head) / (denom * denom)).astype(jnp.bfloat16)
        ddenom_rows = (ddenom.astype(jnp.float32) * segments.astype(jnp.float32)).astype(jnp.bfloat16)
        dquery_feat = dot_last(dnumer_slots, state) + dot_last(ddenom_rows, total)
        dexp = dquery_feat * query_feat
        dquery = dot_last(dexp.astype(jnp.bfloat16), half_dirs) - query.astype(jnp.float32) * jnp.sum(
            dexp, axis=1, keepdims=True
        )
        dstate = dot_rows(query_low, dnumer_slots).astype(jnp.bfloat16)
        dtotal = dot_rows(query_low, ddenom_rows).astype(jnp.bfloat16)
        dkey_feat = dot_last(value_slots, dstate) + dot_last(segments, dtotal)
        dexp = dkey_feat * key_feat
        dkey = dot_last(dexp.astype(jnp.bfloat16), half_dirs) - key.astype(jnp.float32) * jnp.sum(
            dexp, axis=1, keepdims=True
        )
        dvalue = slot_sum(jnp.dot(key_low, dstate, preferred_element_type=jnp.float32), mask)
        outs.append((dquery * scale, dkey * scale, dvalue))
    for part in range(3):
        both = jnp.where(lane_half(outs[0][part].shape), outs[0][part], outs[1][part])
        dqkv_ref[:, pair_cols(part, pair, width)] = both.astype(jnp.bfloat16)


def attend(pairs, scale, tokens, weight, bias, dirs, mask, segments):
    rows, width = tokens.shape
    outs = [jax.ShapeDtypeStruct((rows, 3 * width), jnp.bfloat16), jax.ShapeDtypeStruct((rows, width), jnp.bfloat16)]

    def body(pair, *refs):
        forward_pair(pair, scale, *refs)

    return Work(body, pairs, (tokens, weight, bias, dirs, mask, segments), outs)


def attend_back(pairs, scale, qkv, dcontext, dirs, mask, segments):
    def body(pair, *refs):
        backward_pair(pair, scale, *refs)

    ins = (qkv, dcontext, dirs, mask, segments)
    return Work(body, pairs, ins, [jax.ShapeDtypeStruct(qkv.shape, jnp.bfloat16)])


def pair_directions(directions):
    heads, size, count = directions.shape
    paired = directions.reshape(heads // 2, 2, size, count)
    zero = jnp.zeros_like(paired[:, 0])
    top = jnp.concatenate([paired[:, 0], zero], axis=2)
    low = jnp.concatenate([zero, paired[:, 1]], axis=2)
    return jnp.concatenate([top, low], axis=1)


def pack_small(vectors, rows):
    joined = jnp.concatenate(vectors, axis=-1)
    room = rows * 128 - joined.shape[-1]
    joined = jnp.pad(joined, [(0, 0)] * (joined.ndim - 1) + [(0, room)])
    return joined.reshape(joined.shape[:-1] + (rows, 128))


def unpack_small(packed, sizes):
    flat = packed.reshape(packed.shape[:-2] + (-1,))
    parts, at = [], 0
    for size in sizes:
        parts.append(flat[..., at : at + size])
        at += size
    return parts


def layer_norm(summed, gain_vec, shift_vec):
    centered = summed - jnp.mean(summed, -1, keepdims=True)
    inv_std = lax.rsqrt(jnp.mean(centered * centered, -1, keepdims=True) + EPSILON)
    return centered * inv_std * gain_vec + shift_vec


def matrix_product(left, right):
    return jnp.dot(left, right, preferred_element_type=jnp.float32)


def rows_product(left, right):
    return lax.dot_general(
        left, right, (((0,), (0,)), ((), ())), preferred_element_type=jnp.float32
    )


def back_product(left, right):
    return lax.dot_general(
        left, right, (((1,), (1,)), ((), ())), preferred_element_type=jnp.float32
    )


def column_sum(values_low):
    return jnp.sum(values_low.astype(jnp.float32), axis=0)


def body(
    tokens,
    cotangent,
    qkv_weight,
    qkv_bias,
    proj_weight,
    proj_bias,
    attn_gain,
    attn_shift,
    inner_weight,
    inner_bias,
    outer_weight,
    outer_bias,
    ffn_gain,
    ffn_shift,
    random_dirs,
    seq_lengths,
    deal_order,
):
    groups = lax.axis_size("fsdp")
    row_count, model_width = tokens.shape
    piece_rows = row_count // groups
    deal_row = deal_order[0]
    pick = lambda pieces, order: pieces.at[order].get(mode="promise_in_bounds", unique_indices=True)
    send_tokens = pick(tokens.reshape(groups, piece_rows, model_width), deal_row)
    send_grads = pick(cotangent.reshape(groups, piece_rows, model_width), deal_row)
    replicas = lax.axis_size("replica")
    vectors = (qkv_bias, proj_bias, attn_gain, attn_shift, inner_bias, outer_bias, ffn_gain, ffn_shift)
    sizes = [v.shape[0] for v in vectors]
    weight_qkv, small_all, arrived_x = gather_all(
        groups, replicas, 0, (qkv_weight,), [v[None] for v in vectors], (send_tokens,)
    )
    token_low = arrived_x.reshape(row_count, model_width)
    bias_qkv, bias_proj, gain_attn, shift_attn, bias_inner, bias_outer, gain_ffn, shift_ffn = (
        small_all[:, row, :size].reshape(-1) for row, size in enumerate(sizes)
    )
    lengths_here = seq_lengths[0, 0]
    seq_ends = jnp.cumsum(lengths_here)
    slot_count = lengths_here.shape[0] + 1
    position = lax.iota(jnp.int32, row_count)
    segment = jnp.sum((position[:, None] >= seq_ends[None, :]).astype(jnp.int32), axis=1)
    slot_of = lax.iota(jnp.int32, SLOTS * LANES // 2) // (LANES // 2)
    slot_mask = (segment[:, None] == slot_of[None, :]).astype(jnp.bfloat16)
    segments = (segment[:, None] == lax.iota(jnp.int32, LANES)[None, :]).astype(jnp.bfloat16)
    directions = pair_directions(random_dirs)
    valid_rows = (segment < slot_count - 1).astype(jnp.float32)[:, None]
    head_count, head_dim = (random_dirs.shape[0], random_dirs.shape[1])
    feature_scale = head_dim ** (-0.25)
    pairs = head_count // 2
    weight_proj, weight_inner, weight_outer, arrived_g, qkv_low, context_low = gather_all(
        groups,
        replicas,
        1,
        (proj_weight, inner_weight, outer_weight),
        (),
        (send_grads,),
        attend(pairs, feature_scale, token_low, weight_qkv, bias_qkv[None], directions, slot_mask, segments),
    )
    upstream = arrived_g.reshape(row_count, model_width).astype(jnp.float32)
    attn_out = matrix_product(context_low, weight_proj) + bias_proj
    hidden, first_pull = jax.vjp(
        layer_norm, token_low.astype(jnp.float32) + attn_out, gain_attn, shift_attn
    )
    hidden_low = hidden.astype(jnp.bfloat16)
    inner_act = matrix_product(hidden_low, weight_inner) + bias_inner
    gelu_act, gelu_pull = jax.vjp(partial(jax.nn.gelu, approximate=False), inner_act)
    gelu_low = gelu_act.astype(jnp.bfloat16)
    outer_act = matrix_product(gelu_low, weight_outer) + bias_outer
    normed_out, second_pull = jax.vjp(layer_norm, hidden + outer_act, gain_ffn, shift_ffn)
    result = normed_out * valid_rows
    back_qkv, back_proj, back_inner, back_outer = weight_qkv, weight_proj, weight_inner, weight_outer
    dsecond, grad_gain_ffn, grad_shift_ffn = second_pull(upstream * valid_rows)
    douter_low = dsecond.astype(jnp.bfloat16)
    grad_bias_outer = column_sum(douter_low)
    grad_weight_outer = rows_product(gelu_low, douter_low)
    dinner_low = gelu_pull(back_product(douter_low, back_outer))[0].astype(jnp.bfloat16)
    grad_bias_inner = column_sum(dinner_low)
    grad_weight_inner = rows_product(hidden_low, dinner_low)
    dhidden = dsecond + back_product(dinner_low, back_inner)
    dfirst, grad_gain_attn, grad_shift_attn = first_pull(dhidden)
    dattn_low = dfirst.astype(jnp.bfloat16)
    grad_bias_proj = column_sum(dattn_low)
    grad_weight_proj = rows_product(context_low, dattn_low)
    dcontext = back_product(dattn_low, back_proj)
    out_rows = result.astype(jnp.bfloat16).reshape(groups, piece_rows, model_width)
    sum_wproj, sum_winner, sum_wouter, back_out, dqkv_low = scatter_all(
        groups,
        replicas,
        2,
        [g.astype(jnp.bfloat16) for g in (grad_weight_proj, grad_weight_inner, grad_weight_outer)],
        (),
        (out_rows,),
        attend_back(pairs, feature_scale, qkv_low, dcontext, directions, slot_mask, segments),
    )
    grad_bias_qkv = column_sum(dqkv_low)
    grad_weight_qkv = rows_product(token_low, dqkv_low)
    dtokens = dfirst + back_product(dqkv_low, back_qkv)
    grad_rows = dtokens.astype(jnp.bfloat16).reshape(groups, piece_rows, model_width)
    vector_grads = (
        grad_bias_qkv,
        grad_bias_proj,
        grad_gain_attn,
        grad_shift_attn,
        grad_bias_inner,
        grad_bias_outer,
        grad_gain_ffn,
        grad_shift_ffn,
    )
    small_grads = pack_small([v.reshape(groups, -1) for v in vector_grads], 8)
    sum_wqkv, small_sum, back_grad = scatter_all(
        groups, replicas, 3, [grad_weight_qkv.astype(jnp.bfloat16)], (small_grads,), (grad_rows,)
    )
    sum_bqkv, sum_bproj, sum_gattn, sum_sattn, sum_binner, sum_bouter, sum_gffn, sum_sffn = unpack_small(
        small_sum, sizes
    )
    inverse = jnp.zeros((groups,), jnp.int32).at[deal_row].set(lax.iota(jnp.int32, groups))
    layer_out = pick(back_out, inverse).reshape(row_count, model_width)
    tokens_grad = pick(back_grad, inverse).reshape(row_count, model_width)
    return (
        layer_out,
        tokens_grad,
        sum_wqkv,
        sum_bqkv,
        sum_wproj,
        sum_bproj,
        sum_gattn,
        sum_sattn,
        sum_winner,
        sum_binner,
        sum_wouter,
        sum_bouter,
        sum_gffn,
        sum_sffn,
    )


def solution(mesh):
    return jax.shard_map(
        body,
        mesh=mesh,
        in_specs=(
            P(("replica", "fsdp"), None),
            P(("replica", "fsdp"), None),
            P("fsdp", None),
            P("fsdp"),
            P("fsdp", None),
            P("fsdp"),
            P("fsdp"),
            P("fsdp"),
            P("fsdp", None),
            P("fsdp"),
            P("fsdp", None),
            P("fsdp"),
            P("fsdp"),
            P("fsdp"),
            P(),
            P("replica", "fsdp", None),
            P("replica", None),
        ),
        out_specs=(
            P(("replica", "fsdp"), None),
            P(("replica", "fsdp"), None),
            P("fsdp", None),
            P("fsdp"),
            P("fsdp", None),
            P("fsdp"),
            P("fsdp"),
            P("fsdp"),
            P("fsdp", None),
            P("fsdp"),
            P("fsdp", None),
            P("fsdp"),
            P("fsdp"),
            P("fsdp"),
        ),
        check_vma=False,
    )
```

```python
from functools import partial

import jax
import jax.numpy as jnp
from jax import lax
from jax.experimental import pallas as pl
from jax.experimental.pallas import tpu as pltpu
from jax.sharding import PartitionSpec as P

EPSILON = 1e-06
ANY = pl.BlockSpec(memory_space=pl.ANY)
VMEM = pl.BlockSpec(memory_space=pltpu.VMEM)
MESH = pl.DeviceIdType.MESH
DMA = pltpu.SemaphoreType.DMA


class Place:
    def __init__(self, n, replicas):
        self.n, self.replicas = n, replicas
        self.nz = 4 if n % 8 == 0 else n // 2
        self.ny = n // (2 * self.nz)
        self.chips = n // 2
        self.f = lax.axis_index("fsdp")
        self.r = lax.axis_index("replica")
        self.core = self.f % 2
        chip = self.f // 2
        y, z = chip % self.ny, chip // self.ny
        odd = y % 2
        self.pos = y * self.nz + z * (1 - odd) + (self.nz - 1 - z) * odd
        self.role = self.r % 2

    def dev(self, pos, core):
        pos = (pos + 2 * self.chips) % self.chips
        y, t = pos // self.nz, pos % self.nz
        odd = y % 2
        z = t * (1 - odd) + (self.nz - 1 - t) * odd
        return (z * self.ny + y) * 2 + core

    def peer(self, f):
        return (self.r, f)

    def ring(self, direction):
        return self.peer(self.dev(self.pos + (1 if direction == 0 else -1), self.core))

    def mate(self):
        return self.peer(self.f + 1 - 2 * self.core)

    def across(self):
        return (self.r + 1 - 2 * self.role, self.f)

    def greet(self):
        barrier = pltpu.get_barrier_semaphore()

        @pl.loop(1, self.n)
        def _(k):
            pl.semaphore_signal(barrier, inc=1, device_id=self.peer((self.f + k) % self.n), device_id_type=MESH)

        @pl.loop(1, self.replicas)
        def _(k):
            pl.semaphore_signal(barrier, inc=1, device_id=((self.r + k) % self.replicas, self.f), device_id_type=MESH)

        pl.semaphore_wait(barrier, self.n - 1 + self.replicas - 1)


def remote(src, dst, send, recv, device):
    return pltpu.make_async_remote_copy(
        src_ref=src, dst_ref=dst, send_sem=send, recv_sem=recv, device_id=device, device_id_type=MESH
    )


class Exchange:
    def __init__(self, place, send, recv, sems):
        self.place, self.send, self.recv = place, send, recv
        self.out_sem, self.in_sem, self.own_sem = sems

    def copy(self, target):
        me = self.place.f
        return remote(
            self.send.at[target], self.recv.at[me], self.out_sem, self.in_sem, self.place.peer(target)
        )

    def own(self):
        me = self.place.f
        return pltpu.make_async_copy(self.send.at[me], self.recv.at[me], self.own_sem)

    def start(self):
        self.own().start()

        @pl.loop(1, self.place.n)
        def _(k):
            self.copy((self.place.f + k) % self.place.n).start()

    def trickle(self, index, steps):
        count = -(-(self.place.n - 1) // steps)

        @pl.loop(0, count)
        def _(k):
            offset = 1 + index * count + k

            @pl.when(offset < self.place.n)
            def _():
                self.copy((self.place.f + offset) % self.place.n).start()

    def finish(self):
        rest = self.recv.at[pl.ds(0, self.place.n - 1)]
        pltpu.make_async_copy(rest, rest, self.out_sem).wait()
        pltpu.make_async_copy(rest, rest, self.in_sem).wait()
        self.own().wait()


class Spread(Exchange):
    def copy(self, target):
        return remote(
            self.send, self.recv.at[self.place.f], self.out_sem, self.in_sem, self.place.peer(target)
        )

    def own(self):
        return pltpu.make_async_copy(self.send, self.recv.at[self.place.f], self.own_sem)


class Gather:
    def __init__(self, place, shard, full, sems):
        self.place, self.shard, self.full = place, shard, full
        self.ring_in, self.across_in, self.flat = sems
        self.rows, self.cols = shard.shape
        split = self.rows % 48 == 0 and place.replicas % 2 == 0
        self.third = self.rows // 3 if split else 0
        self.main = self.rows - self.third
        self.half = self.cols // 2

    def box(self, ref, owner, offset, count, direction):
        row = offset if owner is None else owner * self.rows + offset
        if owner is not None or not isinstance(row, int):
            row = pl.multiple_of(row, 8)
        return ref.at[pl.ds(row, count), pl.ds(direction * self.half, self.half)]

    def origin(self, s, direction):
        return self.place.pos - s if direction == 0 else self.place.pos + s

    def ring_copy(self, s, direction, own=False):
        owner = self.place.dev(self.origin(s, direction), self.place.core)
        lead = self.place.role * self.third
        dst = self.box(self.full, owner, lead, self.main, direction)
        src = self.box(self.shard, None, lead, self.main, direction) if own else dst
        return remote(src, dst, self.flat.at[0], self.ring_in.at[s, direction], self.place.ring(direction))

    def mate_copy(self, s, direction, lead, count):
        owner = self.place.dev(self.origin(s, direction), self.place.core)
        part = self.box(self.full, owner, lead, count, direction)
        return remote(part, part, self.flat.at[1], self.flat.at[2], self.place.mate())

    def across_copy(self, s, direction, arriving=False):
        owner = self.place.dev(self.origin(s, direction), self.place.core)
        role = 1 - self.place.role if arriving else self.place.role
        part = self.box(self.full, owner, role * 2 * self.third, self.third, direction)
        return remote(part, part, self.flat.at[3], self.across_in.at[s - 1, direction], self.place.across())

    def own_copy(self):
        row = pl.multiple_of(self.place.f * self.rows, 8)
        return pltpu.make_async_copy(self.shard, self.full.at[pl.ds(row, self.rows)], self.flat.at[4])

    def start(self):
        for direction in range(2):
            self.ring_copy(0, direction, own=True).start()
        row = pl.multiple_of(self.place.f * self.rows, 8)
        remote(
            self.shard, self.full.at[pl.ds(row, self.rows)], self.flat.at[1], self.flat.at[2], self.place.mate()
        ).start()
        self.own_copy().start()

    def step(self, s, last=False):
        for direction in range(2):
            owner = self.place.dev(self.origin(s, direction), self.place.core)
            lead = self.place.role * self.third
            part = self.box(self.full, owner, lead, self.main, direction)
            remote(part, part, self.flat.at[0], self.ring_in.at[s - 1, direction], self.place.ring(direction)).wait_recv()
            if not last:
                self.ring_copy(s, direction).start()
            if self.third:
                self.across_copy(s, direction).start()
            self.mate_copy(s, direction, lead, self.main).start()

    def across_step(self, s):
        if self.third:
            for direction in range(2):
                self.across_copy(s, direction, arriving=True).wait_recv()
                self.mate_copy(s, direction, (1 - self.place.role) * 2 * self.third, self.third).start()

    def wait_rows(self, count, index):
        part = self.full.at[pl.ds(0, count)]
        pltpu.make_async_copy(part, part, self.flat.at[index]).wait()

    def finish(self):
        hops = self.place.chips - 1
        self.wait_rows(hops * self.main, 0)
        self.wait_rows(self.place.chips * self.rows, 1)
        self.wait_rows(self.place.chips * self.rows, 2)
        if self.third:
            self.wait_rows(hops * self.third, 3)
        self.own_copy().wait()


FRONT_BLOCK = (8, 256)


def front_kernel(n, replicas, pairs, scale, vectors, *refs):
    refs = list(refs)
    take = lambda count: [refs.pop(0) for _ in range(count)]
    shards, singles, (send_x, send_g), (dirs, mask, segments) = take(4), take(vectors), take(2), take(3)
    fulls, (small_out, got_x, got_g), (qkv_ref, ctx_ref) = take(4), take(3), take(2)
    packed, bias_row, weight = take(3)
    gather_sems = [take(3) for _ in range(4)]
    spread_sems, x_sems, g_sems, (load_sem,) = take(3), take(3), take(3), take(1)
    place = Place(n, replicas)
    first, *others = [Gather(place, *item) for item in zip(shards, fulls, gather_sems)]
    spread = Spread(place, packed, small_out, spread_sems)
    swap_x = Exchange(place, send_x, got_x, x_sems)
    swap_g = Exchange(place, send_g, got_g, g_sems)
    for row, single in enumerate(singles):
        packed[row : row + 1, : single.shape[1]] = single[...].astype(jnp.float32)
    place.greet()
    hops = place.chips - 1
    first.start()
    spread.start()
    swap_x.own().start()
    swap_x.trickle(0, hops)

    @pl.loop(1, hops)
    def _(s):
        first.step(s)

        @pl.when(s > 1)
        def _():
            first.across_step(s - 1)

        swap_x.trickle(s, hops)

        @pl.when(s == hops // 2 + 1)
        def _():
            for item in others:
                item.start()

    first.step(hops, last=True)
    first.across_step(hops - 1)
    first.across_step(hops)
    swap_g.own().start()
    first.finish()
    load = pltpu.make_async_copy(fulls[0], weight, load_sem)
    load.start()
    spread.finish()
    size = singles[0].shape[1]
    for k in range(n):
        bias_row[0:1, k * size : (k + 1) * size] = small_out[k, 0:1, :size]
    swap_x.finish()
    load.wait()
    steps = max(hops - 1, pairs)

    @pl.loop(0, steps)
    def _(i):
        @pl.when(i < hops - 1)
        def _():
            for item in others:
                item.step(i + 1)

        @pl.when(jnp.logical_and(i > 0, i < hops - 1))
        def _():
            for item in others:
                item.across_step(i)

        swap_g.trickle(i, steps)

        @pl.when(i < pairs)
        def _():
            forward_pair(i, scale, got_x, weight, bias_row, dirs, mask, segments, qkv_ref, ctx_ref)

    for item in others:
        item.step(hops, last=True)
    for item in others:
        item.across_step(hops - 1)
    for item in others:
        item.across_step(hops)
    for item in others:
        item.finish()
    swap_g.finish()


def front(pairs, scale, collective_id, n, replicas, shards, singles, sends, dirs, mask, segments):
    hops = n // 2 - 1
    rows = mask.shape[0]
    width = shards[0].shape[0] * n
    low = jnp.bfloat16
    outs = [jax.ShapeDtypeStruct((n * a.shape[0], a.shape[1]), a.dtype) for a in shards]
    outs += [jax.ShapeDtypeStruct((n,) + FRONT_BLOCK, jnp.float32)]
    outs += [jax.ShapeDtypeStruct(a.shape, a.dtype) for a in sends]
    outs += [jax.ShapeDtypeStruct((rows, 3 * width), low), jax.ShapeDtypeStruct((rows, width), low)]
    scratch = [
        pltpu.VMEM(FRONT_BLOCK, jnp.float32),
        pltpu.VMEM((1, 3 * width), jnp.float32),
        pltpu.VMEM((width, 3 * width), low),
    ]
    scratch += [DMA((hops, 2)), DMA((hops, 2)), DMA((5,))] * 4 + [DMA(())] * 10
    return pl.pallas_call(
        partial(front_kernel, n, replicas, pairs, scale, len(singles)),
        out_shape=outs,
        in_specs=[VMEM] * (4 + len(singles)) + [ANY] * 2 + [VMEM] * 3,
        out_specs=[ANY] * 4 + [VMEM, VMEM, ANY] + [VMEM] * 2,
        scratch_shapes=scratch,
        compiler_params=pltpu.CompilerParams(
            collective_id=collective_id, has_side_effects=True, vmem_limit_bytes=56 << 20
        ),
        name="front",
    )(*shards, *singles, *sends, dirs, mask, segments)


class Work:
    def __init__(self, body=None, count=0, ins=(), outs=()):
        self.body, self.count, self.ins, self.outs = body, count, tuple(ins), tuple(outs)

    def at(self, index, refs):
        if self.count:

            @pl.when(index < self.count)
            def _():
                self.body(index, *refs)

    def rest(self, start, refs):
        if self.count > start:

            @pl.loop(start, self.count)
            def _(index):
                self.body(index, *refs)


class Scatter:
    def __init__(self, place, grad, total, bufs, sems):
        self.place, self.grad, self.total = place, grad, total
        self.own, self.other, self.ringed, self.repl = bufs
        self.own_in, self.core_in, self.ring_in, self.repl_in, self.flat = sems
        self.rows, self.cols = total.shape
        self.half = self.cols // 2

    def rows_of(self, pos, core):
        row = pl.multiple_of(self.place.dev(pos, core) * self.rows, 8)
        return self.grad.at[pl.ds(row, self.rows)]

    def slot(self, pos):
        return (pos + 2 * self.place.chips) % self.place.chips

    def load(self, pos):
        k = self.slot(pos)
        return pltpu.make_async_copy(self.rows_of(pos, self.place.core), self.own.at[k], self.own_in.at[k])

    def give(self, pos):
        k = self.slot(pos)
        return remote(
            self.rows_of(pos, 1 - self.place.core), self.other.at[k], self.flat.at[0], self.core_in.at[k], self.place.mate()
        )

    def start(self):
        def one(k, _):
            pos = self.place.pos + ((k + 2) // 2) * (2 * (k % 2) - 1)
            self.load(pos).start()
            self.give(pos).start()
            return 0

        lax.fori_loop(0, self.place.chips - 1, one, 0)
        self.load(self.place.pos).start()
        self.give(self.place.pos).start()

    def merge(self, pos):
        k = self.slot(pos)
        self.load(pos).wait()
        self.give(pos).wait_recv()
        self.own[k] = (self.own[k].astype(jnp.float32) + self.other[k].astype(jnp.float32)).astype(jnp.bfloat16)

    def target(self, s, direction):
        return self.place.pos - 1 - s if direction == 0 else self.place.pos + 1 + s

    def cols_of(self, direction):
        return pl.ds(direction * self.half, self.half)

    def ring_copy(self, s, direction, first=False):
        cols = self.cols_of(direction)
        if first:
            src = self.own.at[self.slot(self.target(0, direction)), :, cols]
        else:
            src = self.ringed.at[s - 1, :, cols]
        return remote(src, self.ringed.at[s, :, cols], self.flat.at[1], self.ring_in.at[s, direction], self.place.ring(direction))

    def absorb(self, s, direction):
        cols = self.cols_of(direction)
        self.ring_copy(s, direction, first=True).wait_recv()
        k = self.slot(self.target(s + 1, direction))
        self.ringed[s, :, cols] = (
            self.ringed[s, :, cols].astype(jnp.float32) + self.own[k, :, cols].astype(jnp.float32)
        ).astype(jnp.bfloat16)

    def publish(self):
        hops = self.place.chips - 1
        last = self.ringed.at[hops - 1]

        def one(k, _):
            r = (self.place.r + k) % self.place.replicas
            remote(last, self.repl.at[self.place.r], self.flat.at[2], self.repl_in.at[0], (r, self.place.f)).start()
            return 0

        lax.fori_loop(1, self.place.replicas, one, 0)
        self.repl[self.place.r] = self.ringed[hops - 1]

    def finish(self):
        others = self.repl.at[pl.ds(0, self.place.replicas - 1)]
        pltpu.make_async_copy(others, others, self.repl_in.at[0]).wait()
        total = self.repl[0].astype(jnp.float32)
        for r in range(1, self.place.replicas):
            total = total + self.repl[r].astype(jnp.float32)
        self.total[...] = total
        pltpu.make_async_copy(others, others, self.flat.at[2]).wait()
        pltpu.make_async_copy(self.ringed, self.ringed, self.flat.at[1]).wait()
        pltpu.make_async_copy(self.other, self.other, self.flat.at[0]).wait()


def scatter_kernel(n, replicas, weights, spreads, exchanges, work, *refs):
    refs = list(refs)
    take = lambda count: [refs.pop(0) for _ in range(count)]
    grads, small, sends, ins = take(weights), take(spreads), take(exchanges), take(len(work.ins))
    totals, small_total, recvs, outs = take(weights), take(spreads), take(exchanges), take(len(work.outs))
    bufs = [take(4) for _ in range(weights)]
    small_bufs = take(2 * spreads)
    sems = [take(5) for _ in range(weights)]
    small_sems = take(4 * spreads)
    exchange_sems = [take(3) for _ in range(exchanges)]
    place = Place(n, replicas)
    scatters = [Scatter(place, *item) for item in zip(grads, totals, bufs, sems)]
    swaps = [Exchange(place, *item) for item in zip(sends, recvs, exchange_sems)]
    place.greet()
    hops = place.chips - 1
    for item in scatters:
        item.start()
    if spreads:
        small_in, small_group = small_bufs
        small_repl = small_sems[3]
        smalls = Exchange(place, small[0], small_in, small_sems[:3])
        smalls.start()
    for item in scatters:
        item.merge(place.pos - 1)
        item.ring_copy(0, 0, first=True).start()
        item.merge(place.pos + 1)
        item.ring_copy(0, 1, first=True).start()
    for item in swaps:
        item.start()

    @pl.loop(0, hops - 1)
    def _(s):
        work.at(s, ins + outs)
        for item in scatters:

            @pl.when(s < (place.chips - 2) // 2)
            def _():
                item.merge(place.pos - 2 - s)

            @pl.when(s < hops // 2 - 1)
            def _():
                item.merge(place.pos + 2 + s)

            for direction in range(2):
                item.absorb(s, direction)
                item.ring_copy(s + 1, direction).start()

    work.rest(hops - 1, ins + outs)
    if spreads:
        smalls.finish()
        group = small_in[0]
        for k in range(1, n):
            group = group + small_in[k]
        small_group[place.r] = group

        @pl.loop(1, replicas)
        def _(k):
            mine = small_group.at[place.r]
            target = ((place.r + k) % replicas, place.f)
            remote(mine, mine, small_repl.at[0], small_repl.at[1], target).start()

    for item in scatters:
        item.merge(place.pos)
        for direction in range(2):
            item.absorb(hops - 1, direction)
        item.publish()
    if spreads:
        others = small_group.at[pl.ds(0, replicas - 1)]
        pltpu.make_async_copy(others, others, small_repl.at[1]).wait()
        total = small_group[0]
        for r in range(1, replicas):
            total = total + small_group[r]
        small_total[0][...] = total
        pltpu.make_async_copy(others, others, small_repl.at[0]).wait()
    for item in scatters:
        item.finish()
    for item in swaps:
        item.finish()


def scatter_all(n, replicas, collective_id, grads, small, sends, work=Work()):
    chips, hops = n // 2, n // 2 - 1
    outs = [jax.ShapeDtypeStruct((a.shape[0] // n, a.shape[1]), jnp.float32) for a in grads]
    outs += [jax.ShapeDtypeStruct(a.shape[1:], jnp.float32) for a in small]
    wide = [jax.ShapeDtypeStruct(a.shape, a.dtype) for a in sends]
    scratch = []
    for a in grads:
        block = (a.shape[0] // n, a.shape[1])
        scratch += [pltpu.VMEM((count,) + block, jnp.bfloat16) for count in (chips, chips, hops, replicas)]
    for a in small:
        scratch += [pltpu.VMEM(a.shape, jnp.float32), pltpu.VMEM((replicas,) + a.shape[1:], jnp.float32)]
    scratch += [DMA((chips,)), DMA((chips,)), DMA((hops, 2)), DMA((1,)), DMA((3,))] * len(grads)
    scratch += [DMA(()), DMA(()), DMA(()), DMA((2,))] * len(small) + [DMA(()), DMA(()), DMA(())] * len(sends)
    return pl.pallas_call(
        partial(scatter_kernel, n, replicas, len(grads), len(small), len(sends), work),
        out_shape=outs + wide + list(work.outs),
        in_specs=[ANY] * (len(grads) + len(small) + len(sends)) + [VMEM] * len(work.ins),
        out_specs=[VMEM] * len(outs) + [ANY] * len(wide) + [VMEM] * len(work.outs),
        scratch_shapes=scratch,
        compiler_params=pltpu.CompilerParams(
            collective_id=collective_id, has_side_effects=True, vmem_limit_bytes=56 << 20
        ),
        name="scatter_all",
    )(*grads, *small, *sends, *work.ins)


LANES = 128
SLOTS = 6


def lane_half(shape):
    return lax.broadcasted_iota(jnp.int32, shape, 1) < LANES // 2


def dot_rows(left, right):
    return lax.dot_general(left, right, (((0,), (0,)), ((), ())), preferred_element_type=jnp.float32)


def dot_last(left, right):
    return lax.dot_general(left, right, (((1,), (1,)), ((), ())), preferred_element_type=jnp.float32)


def own_half(wide, head):
    turned = pltpu.roll(wide, LANES // 2, 1)
    first = lane_half(wide.shape)
    return jnp.where(first, wide, turned) if head == 0 else jnp.where(first, turned, wide)


def in_slots(wide, head, mask):
    same = own_half(wide, head).astype(jnp.bfloat16)
    return jnp.concatenate([same] * (SLOTS // 2), axis=1) * mask


def slot_sum(wide, mask):
    picked = wide * mask.astype(jnp.float32)
    both = picked[:, :LANES] + picked[:, LANES : 2 * LANES] + picked[:, 2 * LANES :]
    return both + pltpu.roll(both, LANES // 2, 1)


def half_norm(wide, head):
    keep = lane_half(wide.shape) if head == 0 else jnp.logical_not(lane_half(wide.shape))
    return jnp.sum(jnp.where(keep, wide, 0.0), axis=1, keepdims=True)


def pair_cols(part, pair, width):
    return pl.ds(pl.multiple_of(part * width + pair * LANES, LANES), LANES)


def features(low, directions, head):
    count = directions.shape[1] // 2
    project = jnp.dot(low, directions[:, head * count : (head + 1) * count], preferred_element_type=jnp.float32)
    wide = low.astype(jnp.float32)
    return jnp.exp(project - 0.5 * half_norm(wide * wide, head))


def states(key_low, value_wide, head, mask, segments):
    value_slots = in_slots(value_wide, head, mask)
    state = dot_rows(key_low, value_slots).astype(jnp.bfloat16)
    total = dot_rows(key_low, segments).astype(jnp.bfloat16)
    return value_slots, state, total


def readout(query_low, state, total, mask, segments):
    numer = slot_sum(jnp.dot(query_low, state, preferred_element_type=jnp.float32), mask)
    denom = jnp.dot(query_low, total, preferred_element_type=jnp.float32) * segments.astype(jnp.float32)
    return numer, jnp.sum(denom, axis=1, keepdims=True)


def forward_pair(pair, scale, x_ref, w_ref, b_ref, dirs_ref, mask_ref, seg_ref, qkv_ref, ctx_ref):
    width = x_ref.shape[-1]
    rows = x_ref[...].reshape(-1, width)
    parts = []
    for part in range(3):
        cols = pair_cols(part, pair, width)
        act = jnp.dot(rows, w_ref[:, cols], preferred_element_type=jnp.float32) + b_ref[0:1, cols]
        low = (act * scale if part < 2 else act).astype(jnp.bfloat16)
        qkv_ref[:, cols] = low
        parts.append(low)
    query, key, value = parts
    directions = dirs_ref[pair]
    outs = []
    for head in range(2):
        query_low = features(query, directions, head).astype(jnp.bfloat16)
        key_low = features(key, directions, head).astype(jnp.bfloat16)
        _, state, total = states(key_low, value.astype(jnp.float32), head, mask_ref[...], seg_ref[...])
        numer, denom = readout(query_low, state, total, mask_ref[...], seg_ref[...])
        outs.append(numer / denom)
    ctx_ref[:, pair_cols(0, pair, width)] = jnp.where(lane_half(outs[0].shape), outs[0], outs[1]).astype(jnp.bfloat16)


def backward_pair(pair, scale, qkv_ref, dctx_ref, dirs_ref, mask_ref, seg_ref, dqkv_ref):
    width = dctx_ref.shape[1]
    query, key, value = [qkv_ref[:, pair_cols(part, pair, width)] for part in range(3)]
    dctx = dctx_ref[:, pair_cols(0, pair, width)]
    directions = dirs_ref[pair]
    outs = []
    for head in range(2):
        mask, segments = mask_ref[...], seg_ref[...]
        half_dirs = directions[:, head * (directions.shape[1] // 2) : (head + 1) * (directions.shape[1] // 2)]
        query_feat = features(query, directions, head)
        key_feat = features(key, directions, head)
        query_low, key_low = query_feat.astype(jnp.bfloat16), key_feat.astype(jnp.bfloat16)
        value_slots, state, total = states(key_low, value.astype(jnp.float32), head, mask, segments)
        numer, denom = readout(query_low, state, total, mask, segments)
        dnumer_slots = in_slots(dctx / denom, head, mask)
        ddenom = (-half_norm(dctx * numer, head) / (denom * denom)).astype(jnp.bfloat16)
        ddenom_rows = (ddenom.astype(jnp.float32) * segments.astype(jnp.float32)).astype(jnp.bfloat16)
        dquery_feat = dot_last(dnumer_slots, state) + dot_last(ddenom_rows, total)
        dexp = dquery_feat * query_feat
        dquery = dot_last(dexp.astype(jnp.bfloat16), half_dirs) - query.astype(jnp.float32) * jnp.sum(
            dexp, axis=1, keepdims=True
        )
        dstate = dot_rows(query_low, dnumer_slots).astype(jnp.bfloat16)
        dtotal = dot_rows(query_low, ddenom_rows).astype(jnp.bfloat16)
        dkey_feat = dot_last(value_slots, dstate) + dot_last(segments, dtotal)
        dexp = dkey_feat * key_feat
        dkey = dot_last(dexp.astype(jnp.bfloat16), half_dirs) - key.astype(jnp.float32) * jnp.sum(
            dexp, axis=1, keepdims=True
        )
        dvalue = slot_sum(jnp.dot(key_low, dstate, preferred_element_type=jnp.float32), mask)
        outs.append((dquery * scale, dkey * scale, dvalue))
    for part in range(3):
        both = jnp.where(lane_half(outs[0][part].shape), outs[0][part], outs[1][part])
        dqkv_ref[:, pair_cols(part, pair, width)] = both.astype(jnp.bfloat16)


def attend_back(pairs, scale, qkv, dcontext, dirs, mask, segments):
    def body(pair, *refs):
        backward_pair(pair, scale, *refs)

    ins = (qkv, dcontext, dirs, mask, segments)
    return Work(body, pairs, ins, [jax.ShapeDtypeStruct(qkv.shape, jnp.bfloat16)])


def pair_directions(directions):
    heads, size, count = directions.shape
    paired = directions.reshape(heads // 2, 2, size, count)
    zero = jnp.zeros_like(paired[:, 0])
    top = jnp.concatenate([paired[:, 0], zero], axis=2)
    low = jnp.concatenate([zero, paired[:, 1]], axis=2)
    return jnp.concatenate([top, low], axis=1)


def pack_small(vectors, rows):
    joined = jnp.concatenate(vectors, axis=-1)
    room = rows * 128 - joined.shape[-1]
    joined = jnp.pad(joined, [(0, 0)] * (joined.ndim - 1) + [(0, room)])
    return joined.reshape(joined.shape[:-1] + (rows, 128))


def unpack_small(packed, sizes):
    flat = packed.reshape(packed.shape[:-2] + (-1,))
    parts, at = [], 0
    for size in sizes:
        parts.append(flat[..., at : at + size])
        at += size
    return parts


def layer_norm(summed, gain_vec, shift_vec):
    centered = summed - jnp.mean(summed, -1, keepdims=True)
    inv_std = lax.rsqrt(jnp.mean(centered * centered, -1, keepdims=True) + EPSILON)
    return centered * inv_std * gain_vec + shift_vec


def matrix_product(left, right):
    return jnp.dot(left, right, preferred_element_type=jnp.float32)


def rows_product(left, right):
    return lax.dot_general(
        left, right, (((0,), (0,)), ((), ())), preferred_element_type=jnp.float32
    )


def back_product(left, right):
    return lax.dot_general(
        left, right, (((1,), (1,)), ((), ())), preferred_element_type=jnp.float32
    )


def column_sum(values_low):
    return jnp.sum(values_low.astype(jnp.float32), axis=0)


def body(
    tokens,
    cotangent,
    qkv_weight,
    qkv_bias,
    proj_weight,
    proj_bias,
    attn_gain,
    attn_shift,
    inner_weight,
    inner_bias,
    outer_weight,
    outer_bias,
    ffn_gain,
    ffn_shift,
    random_dirs,
    seq_lengths,
    deal_order,
):
    groups = lax.axis_size("fsdp")
    row_count, model_width = tokens.shape
    piece_rows = row_count // groups
    deal_row = deal_order[0]
    pick = lambda pieces, order: pieces.at[order].get(mode="promise_in_bounds", unique_indices=True)
    send_tokens = pick(tokens.reshape(groups, piece_rows, model_width), deal_row)
    send_grads = pick(cotangent.reshape(groups, piece_rows, model_width), deal_row)
    replicas = lax.axis_size("replica")
    vectors = (qkv_bias, proj_bias, attn_gain, attn_shift, inner_bias, outer_bias, ffn_gain, ffn_shift)
    sizes = [v.shape[0] for v in vectors]
    lengths_here = seq_lengths[0, 0]
    seq_ends = jnp.cumsum(lengths_here)
    slot_count = lengths_here.shape[0] + 1
    position = lax.iota(jnp.int32, row_count)
    segment = jnp.sum((position[:, None] >= seq_ends[None, :]).astype(jnp.int32), axis=1)
    slot_of = lax.iota(jnp.int32, SLOTS * LANES // 2) // (LANES // 2)
    slot_mask = (segment[:, None] == slot_of[None, :]).astype(jnp.bfloat16)
    segments = (segment[:, None] == lax.iota(jnp.int32, LANES)[None, :]).astype(jnp.bfloat16)
    directions = pair_directions(random_dirs)
    valid_rows = (segment < slot_count - 1).astype(jnp.float32)[:, None]
    head_count, head_dim = (random_dirs.shape[0], random_dirs.shape[1])
    feature_scale = head_dim ** (-0.25)
    pairs = head_count // 2
    (
        weight_qkv,
        weight_proj,
        weight_inner,
        weight_outer,
        small_all,
        arrived_x,
        arrived_g,
        qkv_low,
        context_low,
    ) = front(
        pairs,
        feature_scale,
        0,
        groups,
        replicas,
        (qkv_weight, proj_weight, inner_weight, outer_weight),
        [v[None] for v in vectors],
        (send_tokens, send_grads),
        directions,
        slot_mask,
        segments,
    )
    token_low = arrived_x.reshape(row_count, model_width)
    upstream = arrived_g.reshape(row_count, model_width).astype(jnp.float32)
    _, bias_proj, gain_attn, shift_attn, bias_inner, bias_outer, gain_ffn, shift_ffn = (
        small_all[:, row, :size].reshape(-1) for row, size in enumerate(sizes)
    )
    attn_out = matrix_product(context_low, weight_proj) + bias_proj
    hidden, first_pull = jax.vjp(
        layer_norm, token_low.astype(jnp.float32) + attn_out, gain_attn, shift_attn
    )
    hidden_low = hidden.astype(jnp.bfloat16)
    inner_act = matrix_product(hidden_low, weight_inner) + bias_inner
    gelu_act, gelu_pull = jax.vjp(partial(jax.nn.gelu, approximate=False), inner_act)
    gelu_low = gelu_act.astype(jnp.bfloat16)
    outer_act = matrix_product(gelu_low, weight_outer) + bias_outer
    normed_out, second_pull = jax.vjp(layer_norm, hidden + outer_act, gain_ffn, shift_ffn)
    result = normed_out * valid_rows
    back_qkv, back_proj, back_inner, back_outer = weight_qkv, weight_proj, weight_inner, weight_outer
    dsecond, grad_gain_ffn, grad_shift_ffn = second_pull(upstream * valid_rows)
    douter_low = dsecond.astype(jnp.bfloat16)
    grad_bias_outer = column_sum(douter_low)
    grad_weight_outer = rows_product(gelu_low, douter_low)
    dinner_low = gelu_pull(back_product(douter_low, back_outer))[0].astype(jnp.bfloat16)
    grad_bias_inner = column_sum(dinner_low)
    grad_weight_inner = rows_product(hidden_low, dinner_low)
    dhidden = dsecond + back_product(dinner_low, back_inner)
    dfirst, grad_gain_attn, grad_shift_attn = first_pull(dhidden)
    dattn_low = dfirst.astype(jnp.bfloat16)
    grad_bias_proj = column_sum(dattn_low)
    grad_weight_proj = rows_product(context_low, dattn_low)
    dcontext = back_product(dattn_low, back_proj)
    out_rows = result.astype(jnp.bfloat16).reshape(groups, piece_rows, model_width)
    sum_wproj, sum_winner, sum_wouter, back_out, dqkv_low = scatter_all(
        groups,
        replicas,
        2,
        [g.astype(jnp.bfloat16) for g in (grad_weight_proj, grad_weight_inner, grad_weight_outer)],
        (),
        (out_rows,),
        attend_back(pairs, feature_scale, qkv_low, dcontext, directions, slot_mask, segments),
    )
    grad_bias_qkv = column_sum(dqkv_low)
    grad_weight_qkv = rows_product(token_low, dqkv_low)
    dtokens = dfirst + back_product(dqkv_low, back_qkv)
    grad_rows = dtokens.astype(jnp.bfloat16).reshape(groups, piece_rows, model_width)
    vector_grads = (
        grad_bias_qkv,
        grad_bias_proj,
        grad_gain_attn,
        grad_shift_attn,
        grad_bias_inner,
        grad_bias_outer,
        grad_gain_ffn,
        grad_shift_ffn,
    )
    small_grads = pack_small([v.reshape(groups, -1) for v in vector_grads], 8)
    sum_wqkv, small_sum, back_grad = scatter_all(
        groups, replicas, 3, [grad_weight_qkv.astype(jnp.bfloat16)], (small_grads,), (grad_rows,)
    )
    sum_bqkv, sum_bproj, sum_gattn, sum_sattn, sum_binner, sum_bouter, sum_gffn, sum_sffn = unpack_small(
        small_sum, sizes
    )
    inverse = jnp.zeros((groups,), jnp.int32).at[deal_row].set(lax.iota(jnp.int32, groups))
    layer_out = pick(back_out, inverse).reshape(row_count, model_width)
    tokens_grad = pick(back_grad, inverse).reshape(row_count, model_width)
    return (
        layer_out,
        tokens_grad,
        sum_wqkv,
        sum_bqkv,
        sum_wproj,
        sum_bproj,
        sum_gattn,
        sum_sattn,
        sum_winner,
        sum_binner,
        sum_wouter,
        sum_bouter,
        sum_gffn,
        sum_sffn,
    )


def solution(mesh):
    return jax.shard_map(
        body,
        mesh=mesh,
        in_specs=(
            P(("replica", "fsdp"), None),
            P(("replica", "fsdp"), None),
            P("fsdp", None),
            P("fsdp"),
            P("fsdp", None),
            P("fsdp"),
            P("fsdp"),
            P("fsdp"),
            P("fsdp", None),
            P("fsdp"),
            P("fsdp", None),
            P("fsdp"),
            P("fsdp"),
            P("fsdp"),
            P(),
            P("replica", "fsdp", None),
            P("replica", None),
        ),
        out_specs=(
            P(("replica", "fsdp"), None),
            P(("replica", "fsdp"), None),
            P("fsdp", None),
            P("fsdp"),
            P("fsdp", None),
            P("fsdp"),
            P("fsdp"),
            P("fsdp"),
            P("fsdp", None),
            P("fsdp"),
            P("fsdp", None),
            P("fsdp"),
            P("fsdp"),
            P("fsdp"),
        ),
        check_vma=False,
    )
```
